128 devices in a mesh: series: 16 (over z, x), tm: 8 (over y, core).
Axes of the slice: x: 4, y: 4, z: 4, core: 2. Of those that a mesh axis runs over, the one named last changes fastest.
Arguments:
- data: bfloat16 [65536, 4096], P('series', 'tm'), may hold values from -24 to 24
- factors_init: bfloat16 [4096, 256], P('tm'), may hold values from -6 to 6
Outputs:
- loadings: bfloat16 [65536, 256], P('series')
- factors: bfloat16 [4096, 256], P('tm')
- innovations: float32 [4096, 256], P('tm')
- transition: float32 [256, 256], replicated
- residual_share: float32 [], replicated
The draws below stay inside these ranges and needn't reach their ends.
All inputs are finite; a program needn't handle non-finite values.
Results may differ from the reference program's by a relative error of at most 0.015.
Values may be sent and summed in bfloat16 or wider, within the bound.
A program may use at most 128 MiB of HBM per device.

```python
import math
import jax
import jax.numpy as jnp
from jax import lax

FACTORS = 256
ITERS = 3
SERIES = 65536
TIMES = 4096


def draw_data(key, part):
    noise_key, row_key, column_key = jax.random.split(key, 3)
    series_place = jnp.arange(SERIES, dtype=jnp.float32)[:, None] / float(max(SERIES - 1, 1))
    row_random = jnp.exp(jax.random.uniform(row_key, (SERIES, 1), jnp.float32, math.log(0.7), math.log(1.4)))
    row_ramp = jnp.exp(math.log(0.4) + series_place * (math.log(2.4) - math.log(0.4)))
    row_scale = row_ramp * row_random
    column_scale = jnp.exp(jax.random.uniform(column_key, (1, TIMES), jnp.float32, math.log(0.6), math.log(1.6)))
    noise = jnp.clip(jax.random.normal(noise_key, (SERIES, TIMES), jnp.float32), -4.0, 4.0)
    values = row_scale * column_scale * noise
    return values.astype(jnp.bfloat16)


def levels(own_key, extent, cuts, low, largest):
    gain = 1.0
    for position, parts in cuts:
        draws = jax.random.uniform(jax.random.fold_in(jax.random.fold_in(own_key, 6), position), (parts,), jnp.float32, low / len(cuts), largest / len(cuts))
        gain = gain * jnp.repeat(jnp.exp(draws), extent[position] // parts).reshape((-1,) + (1,) * (len(extent) - 1 - position))
    return gain


def bell_draw(rng, dims, spread, bound, cuts=(), kind=jnp.bfloat16):
    entries = spread * jax.random.normal(rng, dims, jnp.float32)
    if cuts:
        entries = entries * levels(rng, dims, cuts, -0.22, 0.18)
    return jnp.clip(entries, -bound, bound).astype(kind)


def setup_inputs(seed: int = 0) -> dict:
    arg_keys = jax.random.split(jax.random.key(seed), 3)
    data = draw_data(jax.random.fold_in(arg_keys[2], 71), 0)
    factors_init = bell_draw(arg_keys[1], (TIMES, FACTORS), 1.0, 6.0, ((0, 8),))
    return {"data": data, "factors_init": factors_init}


RIDGE = 0.01

def regularized_inverse(gram):
    gram_size = gram.shape[0]
    identity = jnp.eye(gram_size, dtype=gram.dtype)
    cholesky_factor = jnp.linalg.cholesky(gram + RIDGE * identity)
    return jax.scipy.linalg.cho_solve((cholesky_factor, True), identity)

def column_gram(left, right):
    return lax.dot_general(left.astype(jnp.float32), right.astype(jnp.float32), (((0,), (0,)), ((), ())), preferred_element_type=jnp.float32)

def reference(data, factors_init):
    precise = lax.Precision.HIGHEST
    factors = factors_init
    loadings = None
    for sweep_index in range(ITERS):
        gram_factors = column_gram(factors, factors)
        projection = jnp.dot(data.astype(jnp.float32), factors.astype(jnp.float32), preferred_element_type=jnp.float32)
        loadings = jnp.dot(projection, regularized_inverse(gram_factors), precision=precise).astype(jnp.bfloat16)
        gram_loadings = column_gram(loadings, loadings)
        cross = column_gram(data, loadings)
        factors = jnp.dot(cross, regularized_inverse(gram_loadings), precision=precise).astype(jnp.bfloat16)
    factors_wide = factors.astype(jnp.float32)
    earlier = factors_wide[:-1]
    later_rows = factors_wide[1:]
    lagged = lax.dot_general(later_rows.astype(jnp.float32), earlier.astype(jnp.float32), (((0,), (0,)), ((), ())), precision=precise, preferred_element_type=jnp.float32)
    base_gram = lax.dot_general(earlier.astype(jnp.float32), earlier.astype(jnp.float32), (((0,), (0,)), ((), ())), precision=precise, preferred_element_type=jnp.float32)
    transition = jnp.dot(lagged, regularized_inverse(base_gram), precision=precise)
    predicted = lax.dot_general(earlier.astype(jnp.float32), transition.astype(jnp.float32), (((1,), (1,)), ((), ())), precision=precise, preferred_element_type=jnp.float32)
    innovations = jnp.concatenate([factors_wide[:1], later_rows - predicted], axis=0)
    fitted = lax.dot_general(loadings.astype(jnp.float32), factors.astype(jnp.float32), (((1,), (1,)), ((), ())), preferred_element_type=jnp.float32)
    data_wide = data.astype(jnp.float32)
    residual_sum = jnp.sum(jnp.square(data_wide - fitted))
    data_sum = jnp.sum(jnp.square(data_wide))
    return (loadings, factors, innovations, transition, residual_sum / data_sum)
```

```python
import jax
import jax.numpy as jnp
from jax import lax
from jax.experimental import pallas as pl
from jax.experimental.pallas import tpu as pltpu
from jax.sharding import PartitionSpec as P

ITERS = 3


RIDGE = 0.01


def sent_to_all(shard, axis):
    copies = jnp.broadcast_to(shard, (lax.axis_size(axis), *shard.shape))
    return lax.all_to_all(copies, axis, split_axis=0, concat_axis=0, tiled=True)


def taken_together(shard, axis):
    everything = sent_to_all(shard, axis)
    return jnp.sum(everything, axis=0)


def packed_total(arrays, axis):
    ends = [0]
    for a in arrays:
        ends.append(ends[-1] + a.size)
    running = taken_together(jnp.concatenate([a.ravel() for a in arrays]), axis)
    return tuple((running[b:e].reshape(a.shape) for a, b, e in zip(arrays, ends, ends[1:])))


def in_blocks(shard, dim, length):
    dims = shard.shape
    tiles = shard.reshape(*dims[:dim], length, dims[dim] // length, *dims[dim + 1 :])
    return jnp.moveaxis(tiles, dim, 0)


def sum_at_owner(shard, axis, dim):
    tiles = in_blocks(shard, dim, lax.axis_size(axis))
    arrived = lax.all_to_all(tiles, axis, split_axis=0, concat_axis=0, tiled=True)
    return arrived.sum(axis=0)


def laid_out(tiles, dim):
    dims = list(tiles.shape[1:])
    dims[dim] *= tiles.shape[0]
    return jnp.moveaxis(tiles, 0, dim).reshape(dims)


def collect(shard, axis, dim):
    tiles = sent_to_all(shard, axis)
    return laid_out(tiles, dim)


def passed_along(block, axis, distance):
    devices = range(lax.axis_size(axis))
    route = [(i - distance, i) for i in devices if i - distance in devices]
    return lax.ppermute(block, axis, route)


def in_one(arrays, axis):
    ravelled, at, gathered = (jnp.concatenate([a.reshape(-1) for a in arrays]), 0, [])
    running = lax.psum(ravelled, axis)
    for a in arrays:
        gathered.append(running[at : at + a.size].reshape(a.shape))
        at += a.size
    return tuple(gathered)


def inverse_kernel(g_ref, out_ref, a_ref, x_ref, e_ref):
    n = g_ref.shape[0]
    rows = lax.broadcasted_iota(jnp.int32, (n, n), 0)
    cols = lax.broadcasted_iota(jnp.int32, (n, n), 1)
    diagonal = rows == cols
    gram = g_ref[...] + jnp.where(diagonal, RIDGE, 0.0)
    masked = jnp.where(diagonal, gram, 0.0)
    down = lax.rsqrt(jnp.sum(masked, axis=1, keepdims=True))
    across = lax.rsqrt(jnp.sum(masked, axis=0, keepdims=True))
    scaled = gram * down * across
    a_ref[...] = scaled
    bound = jnp.max(jnp.sum(jnp.abs(scaled), axis=0, keepdims=True))
    alpha = 1.9 / bound
    start = jnp.where(diagonal, alpha, 0.0)
    x_ref[...] = start
    e_ref[...] = jnp.where(diagonal, 1.0, 0.0) - alpha * scaled

    def narrow(left, right):
        return jnp.dot(
            left.astype(jnp.bfloat16),
            right.astype(jnp.bfloat16),
            preferred_element_type=jnp.float32,
        )

    def wide(left, right):
        return jnp.dot(
            left, right, precision=lax.Precision.HIGHEST, preferred_element_type=jnp.float32
        )

    def squaring(carry):
        step, _ = carry
        for _ in range(2):
            error = e_ref[...]
            guess = x_ref[...]
            e_ref[...] = narrow(error, error)
            x_ref[...] = guess + narrow(guess, error)
        final = e_ref[...]
        return step + 1, jnp.sum(final * final)

    lax.while_loop(
        lambda c: jnp.logical_and(c[0] < 10, jnp.logical_and(c[1] > 1e-2, c[1] < 1e6)),
        squaring,
        (0, jnp.float32(1.0)),
    )

    def residual():
        error = jnp.where(diagonal, 1.0, 0.0) - wide(a_ref[...], x_ref[...])
        e_ref[...] = error
        return jnp.max(jnp.abs(error))

    def refine(carry):
        step, _ = carry
        worst = residual()
        guess = x_ref[...]
        x_ref[...] = guess + narrow(guess, e_ref[...])
        return step + 1, worst

    _, worst = lax.while_loop(
        lambda c: jnp.logical_and(c[0] < 8, jnp.logical_not(c[1] < 5e-4)),
        refine,
        (0, jnp.float32(1.0)),
    )

    @pl.when(jnp.logical_not(worst < 5e-4))
    def _():
        x_ref[...] = jnp.where(diagonal, alpha, 0.0)

        def newton(carry):
            step, _ = carry
            error = residual()
            guess = x_ref[...]
            x_ref[...] = guess + wide(guess, e_ref[...])
            return step + 1, error

        lax.while_loop(
            lambda c: jnp.logical_and(c[0] < 48, jnp.logical_not(c[1] < 5e-4)),
            newton,
            (0, jnp.float32(1.0)),
        )

    out_ref[...] = x_ref[...] * down * across


def regularized_inverse(gram):
    n = gram.shape[0]
    square = pltpu.VMEM((n, n), jnp.float32)
    return pl.pallas_call(
        inverse_kernel,
        out_shape=jax.ShapeDtypeStruct((n, n), jnp.float32),
        in_specs=[pl.BlockSpec(memory_space=pltpu.VMEM)],
        out_specs=pl.BlockSpec(memory_space=pltpu.VMEM),
        scratch_shapes=[square] * 3,
        compiler_params=pltpu.CompilerParams(vmem_limit_bytes=16 * 1024 * 1024),
        name="inverse",
    )(gram)


def column_gram(left, right):
    return lax.dot_general(
        left, right, (((0,), (0,)), ((), ())), preferred_element_type=jnp.float32
    )


def body(data, factors_init):
    precise = lax.Precision.HIGHEST
    factors = factors_init
    data_squares = jnp.sum(jnp.square(data.astype(jnp.float32)))
    loadings = None
    cross = None
    gram_loadings = None
    data_total = None
    for sweep_index in range(ITERS):
        gram_part = column_gram(factors, factors)
        gram_factors, data_block = packed_total((gram_part, data_squares), "tm")
        current = factors
        projection = sum_at_owner(
            jnp.dot(data, current, preferred_element_type=jnp.float32), "tm", 0
        )
        loading_share = jnp.dot(
            projection, regularized_inverse(gram_factors), precision=precise
        ).astype(jnp.bfloat16)
        loadings = collect(loading_share, "tm", 0)
        loading_part = column_gram(loadings, loadings)
        cross_part = column_gram(data, loadings)
        gram_loadings, cross, data_total = lax.psum(
            (loading_part, cross_part, data_block), "series"
        )
        factors = jnp.dot(cross, regularized_inverse(gram_loadings), precision=precise).astype(
            jnp.bfloat16
        )
    previous = passed_along(factors[-1:], "tm", 1)
    earlier = jnp.concatenate([previous, factors[:-1]], axis=0)
    lagged_part = column_gram(factors, earlier)
    base_part = column_gram(earlier, earlier)
    own_gram = column_gram(factors, factors)
    factors_wide = factors.astype(jnp.float32)
    scalar_part = jnp.sum(gram_loadings * own_gram) - 2.0 * jnp.sum(factors_wide * cross)
    lagged, base_gram, expanded = in_one((lagged_part, base_part, scalar_part), "tm")
    residual_total = data_total + expanded
    transition = jnp.dot(lagged, regularized_inverse(base_gram), precision=precise)
    predicted = lax.dot_general(
        earlier.astype(jnp.float32),
        transition,
        (((1,), (1,)), ((), ())),
        precision=precise,
        preferred_element_type=jnp.float32,
    )
    innovations = factors.astype(jnp.float32) - predicted
    residual_share = residual_total / data_total
    return (loadings, factors, innovations, transition, residual_share)


def solution(mesh):
    return jax.shard_map(
        body,
        mesh=mesh,
        in_specs=(P("series", "tm"), P("tm", None)),
        out_specs=(P("series", None), P("tm", None), P("tm", None), P(), P()),
        check_vma=False,
    )
```

```python
import jax
import jax.numpy as jnp
from jax import lax
from jax.experimental import pallas as pl
from jax.experimental.pallas import tpu as pltpu
from jax.sharding import PartitionSpec as P

ITERS = 3


RIDGE = 0.01


def sent_to_all(shard, axis):
    copies = jnp.broadcast_to(shard, (lax.axis_size(axis), *shard.shape))
    return lax.all_to_all(copies, axis, split_axis=0, concat_axis=0, tiled=True)


def taken_together(shard, axis):
    everything = sent_to_all(shard, axis)
    return jnp.sum(everything, axis=0)


def packed_total(arrays, axis):
    ends = [0]
    for a in arrays:
        ends.append(ends[-1] + a.size)
    running = taken_together(jnp.concatenate([a.ravel() for a in arrays]), axis)
    return tuple((running[b:e].reshape(a.shape) for a, b, e in zip(arrays, ends, ends[1:])))


def in_blocks(shard, dim, length):
    dims = shard.shape
    tiles = shard.reshape(*dims[:dim], length, dims[dim] // length, *dims[dim + 1 :])
    return jnp.moveaxis(tiles, dim, 0)


def sum_at_owner(shard, axis, dim):
    tiles = in_blocks(shard, dim, lax.axis_size(axis))
    arrived = lax.all_to_all(tiles, axis, split_axis=0, concat_axis=0, tiled=True)
    return arrived.sum(axis=0)


def laid_out(tiles, dim):
    dims = list(tiles.shape[1:])
    dims[dim] *= tiles.shape[0]
    return jnp.moveaxis(tiles, 0, dim).reshape(dims)


def collect(shard, axis, dim):
    tiles = sent_to_all(shard, axis)
    return laid_out(tiles, dim)


def passed_along(block, axis, distance):
    devices = range(lax.axis_size(axis))
    route = [(i - distance, i) for i in devices if i - distance in devices]
    return lax.ppermute(block, axis, route)


def in_one(arrays, axis):
    ravelled, at, gathered = (jnp.concatenate([a.reshape(-1) for a in arrays]), 0, [])
    running = lax.psum(ravelled, axis)
    for a in arrays:
        gathered.append(running[at : at + a.size].reshape(a.shape))
        at += a.size
    return tuple(gathered)


def inverse_kernel(g_ref, out_ref, a_ref, x_ref, e_ref):
    n = g_ref.shape[0]
    rows = lax.broadcasted_iota(jnp.int32, (n, n), 0)
    cols = lax.broadcasted_iota(jnp.int32, (n, n), 1)
    diagonal = rows == cols
    gram = g_ref[...] + jnp.where(diagonal, RIDGE, 0.0)
    masked = jnp.where(diagonal, gram, 0.0)
    down = lax.rsqrt(jnp.sum(masked, axis=1, keepdims=True))
    across = lax.rsqrt(jnp.sum(masked, axis=0, keepdims=True))
    scaled = gram * down * across
    a_ref[...] = scaled
    bound = jnp.max(jnp.sum(jnp.abs(scaled), axis=0, keepdims=True))
    alpha = 1.9 / bound
    start = jnp.where(diagonal, alpha, 0.0)
    x_ref[...] = start
    e_ref[...] = jnp.where(diagonal, 1.0, 0.0) - alpha * scaled

    def narrow(left, right):
        return jnp.dot(
            left.astype(jnp.bfloat16),
            right.astype(jnp.bfloat16),
            preferred_element_type=jnp.float32,
        )

    def wide(left, right):
        return jnp.dot(
            left, right, precision=lax.Precision.HIGHEST, preferred_element_type=jnp.float32
        )

    def squaring(carry):
        step, _ = carry
        for _ in range(2):
            error = e_ref[...]
            guess = x_ref[...]
            e_ref[...] = narrow(error, error)
            x_ref[...] = guess + narrow(guess, error)
        final = e_ref[...]
        return step + 1, jnp.sum(final * final)

    lax.while_loop(
        lambda c: jnp.logical_and(c[0] < 10, jnp.logical_and(c[1] > 1e-2, c[1] < 1e3)),
        squaring,
        (0, jnp.float32(1.0)),
    )

    def residual():
        error = jnp.where(diagonal, 1.0, 0.0) - wide(a_ref[...], x_ref[...])
        e_ref[...] = error
        return jnp.max(jnp.abs(error))

    def refine(carry):
        step, _ = carry
        worst = residual()
        guess = x_ref[...]
        x_ref[...] = guess + narrow(guess, e_ref[...])
        return step + 1, worst

    _, worst = lax.while_loop(
        lambda c: jnp.logical_and(c[0] < 8, jnp.logical_and(c[1] >= 5e-4, c[1] < 2.0)),
        refine,
        (0, jnp.float32(1.0)),
    )

    @pl.when(worst >= 5e-4)
    def _():
        x_ref[...] = jnp.where(diagonal, alpha, 0.0)

        def newton(carry):
            step, _ = carry
            error = residual()
            guess = x_ref[...]
            x_ref[...] = guess + wide(guess, e_ref[...])
            return step + 1, error

        lax.while_loop(
            lambda c: jnp.logical_and(c[0] < 48, c[1] >= 5e-4),
            newton,
            (0, jnp.float32(1.0)),
        )

    out_ref[...] = x_ref[...] * down * across


def regularized_inverse(gram):
    n = gram.shape[0]
    square = pltpu.VMEM((n, n), jnp.float32)
    return pl.pallas_call(
        inverse_kernel,
        out_shape=jax.ShapeDtypeStruct((n, n), jnp.float32),
        in_specs=[pl.BlockSpec(memory_space=pltpu.VMEM)],
        out_specs=pl.BlockSpec(memory_space=pltpu.VMEM),
        scratch_shapes=[square] * 3,
        compiler_params=pltpu.CompilerParams(vmem_limit_bytes=16 * 1024 * 1024),
        name="inverse",
    )(gram)


def column_gram(left, right):
    return lax.dot_general(
        left, right, (((0,), (0,)), ((), ())), preferred_element_type=jnp.float32
    )


def body(data, factors_init):
    precise = lax.Precision.HIGHEST
    factors = factors_init
    data_squares = jnp.sum(jnp.square(data.astype(jnp.float32)))
    loadings = None
    cross = None
    gram_loadings = None
    data_total = None
    for sweep_index in range(ITERS):
        gram_part = column_gram(factors, factors)
        gram_factors, data_block = packed_total((gram_part, data_squares), "tm")
        current = factors
        projection = sum_at_owner(
            jnp.dot(data, current, preferred_element_type=jnp.float32), "tm", 0
        )
        loading_share = jnp.dot(
            projection, regularized_inverse(gram_factors), precision=precise
        ).astype(jnp.bfloat16)
        loadings = collect(loading_share, "tm", 0)
        loading_part = column_gram(loadings, loadings)
        cross_part = column_gram(data, loadings)
        gram_loadings, cross, data_total = lax.psum(
            (loading_part, cross_part, data_block), "series"
        )
        factors = jnp.dot(cross, regularized_inverse(gram_loadings), precision=precise).astype(
            jnp.bfloat16
        )
    previous = passed_along(factors[-1:], "tm", 1)
    earlier = jnp.concatenate([previous, factors[:-1]], axis=0)
    lagged_part = column_gram(factors, earlier)
    base_part = column_gram(earlier, earlier)
    own_gram = column_gram(factors, factors)
    factors_wide = factors.astype(jnp.float32)
    scalar_part = jnp.sum(gram_loadings * own_gram) - 2.0 * jnp.sum(factors_wide * cross)
    lagged, base_gram, expanded = in_one((lagged_part, base_part, scalar_part), "tm")
    residual_total = data_total + expanded
    transition = jnp.dot(lagged, regularized_inverse(base_gram), precision=precise)
    predicted = lax.dot_general(
        earlier.astype(jnp.float32),
        transition,
        (((1,), (1,)), ((), ())),
        precision=precise,
        preferred_element_type=jnp.float32,
    )
    innovations = factors.astype(jnp.float32) - predicted
    residual_share = residual_total / data_total
    return (loadings, factors, innovations, transition, residual_share)


def solution(mesh):
    return jax.shard_map(
        body,
        mesh=mesh,
        in_specs=(P("series", "tm"), P("tm", None)),
        out_specs=(P("series", None), P("tm", None), P("tm", None), P(), P()),
        check_vma=False,
    )
```

```python
import functools

import jax
import jax.numpy as jnp
from jax import lax
from jax.experimental import pallas as pl
from jax.experimental.pallas import tpu as pltpu
from jax.sharding import PartitionSpec as P

ITERS = 3
RIDGE = 0.01
MESH = pl.DeviceIdType.MESH
F32 = jnp.float32
BF16 = jnp.bfloat16
DMA = pltpu.SemaphoreType.DMA


def narrow(left, right):
    return jnp.dot(left.astype(BF16), right.astype(BF16), preferred_element_type=F32)


def wide(left, right):
    return jnp.dot(left, right, precision=lax.Precision.HIGHEST, preferred_element_type=F32)


def column_gram(left, right):
    return lax.dot_general(left, right, (((0,), (0,)), ((), ())), preferred_element_type=F32)


def inverse_of(g_ref, a_ref, x_ref, e_ref):
    n = g_ref.shape[0]
    rows = lax.broadcasted_iota(jnp.int32, (n, n), 0)
    cols = lax.broadcasted_iota(jnp.int32, (n, n), 1)
    diagonal = rows == cols
    gram = g_ref[...] + jnp.where(diagonal, RIDGE, 0.0)
    masked = jnp.where(diagonal, gram, 0.0)
    down = lax.rsqrt(jnp.sum(masked, axis=1, keepdims=True))
    across = lax.rsqrt(jnp.sum(masked, axis=0, keepdims=True))
    scaled = gram * down * across
    a_ref[...] = scaled
    bound = jnp.max(jnp.sum(jnp.abs(scaled), axis=0, keepdims=True))
    alpha = 1.9 / bound
    start = jnp.where(diagonal, alpha, 0.0)
    x_ref[...] = start
    e_ref[...] = jnp.where(diagonal, 1.0, 0.0) - alpha * scaled

    def squaring(carry):
        step, _ = carry
        for _ in range(2):
            error = e_ref[...]
            guess = x_ref[...]
            e_ref[...] = narrow(error, error)
            x_ref[...] = guess + narrow(guess, error)
        final = e_ref[...]
        return step + 1, jnp.sum(final * final)

    lax.while_loop(
        lambda c: jnp.logical_and(c[0] < 10, jnp.logical_and(c[1] > 1e-2, c[1] < 1e3)),
        squaring,
        (0, jnp.float32(1.0)),
    )

    def residual():
        error = jnp.where(diagonal, 1.0, 0.0) - wide(a_ref[...], x_ref[...])
        e_ref[...] = error
        return jnp.max(jnp.abs(error))

    def refine(carry):
        step, _ = carry
        worst = residual()
        guess = x_ref[...]
        x_ref[...] = guess + narrow(guess, e_ref[...])
        return step + 1, worst

    _, worst = lax.while_loop(
        lambda c: jnp.logical_and(c[0] < 8, jnp.logical_and(c[1] >= 5e-4, c[1] < 2.0)),
        refine,
        (0, jnp.float32(1.0)),
    )

    @pl.when(worst >= 5e-4)
    def _():
        x_ref[...] = jnp.where(diagonal, alpha, 0.0)

        def newton(carry):
            step, _ = carry
            error = residual()
            guess = x_ref[...]
            x_ref[...] = guess + wide(guess, e_ref[...])
            return step + 1, error

        lax.while_loop(
            lambda c: jnp.logical_and(c[0] < 48, c[1] >= 5e-4),
            newton,
            (0, jnp.float32(1.0)),
        )

    return x_ref[...] * down * across


def solve_kernel(g_ref, m_ref, out_ref, a_ref, x_ref, e_ref):
    inverse = inverse_of(g_ref, a_ref, x_ref, e_ref)
    out_ref[...] = wide(m_ref[...], inverse).astype(out_ref.dtype)


def in_vmem(count):
    return [pl.BlockSpec(memory_space=pltpu.VMEM)] * count


def solve(gram, rows):
    square = pltpu.VMEM(gram.shape, F32)
    return pl.pallas_call(
        solve_kernel,
        out_shape=jax.ShapeDtypeStruct(rows.shape, BF16),
        in_specs=in_vmem(2),
        out_specs=in_vmem(1)[0],
        scratch_shapes=[square] * 3,
        compiler_params=pltpu.CompilerParams(vmem_limit_bytes=16 * 1024 * 1024),
        name="solve",
    )(gram, rows)


class Place:
    def __init__(self):
        self.p = lax.axis_index("series")
        self.t = lax.axis_index("tm")
        self.planes = lax.axis_size("series")
        self.times = lax.axis_size("tm")
        self.ring = self.times // 2
        self.y = lax.div(self.t, 2)
        self.c = lax.rem(self.t, 2)
        self.partner = self.t + 1 - 2 * self.c

    def ring_at(self, distance):
        return lax.rem(self.y + distance, self.ring)

    def time_of(self, y):
        return 2 * y + self.c

    def copy(self, src, dst, send, recv, p=None, t=None):
        return pltpu.make_async_remote_copy(
            src_ref=src,
            dst_ref=dst,
            send_sem=send,
            recv_sem=recv,
            device_id=(self.p if p is None else p, self.t if t is None else t),
            device_id_type=MESH,
        )

    def greet(self, others):
        barrier = pltpu.get_barrier_semaphore()
        for p, t in others:
            pl.semaphore_signal(barrier, inc=1, device_id=(p, t), device_id_type=MESH)
        pl.semaphore_wait(barrier, len(others))

    def plane_others(self):
        return [(lax.rem(self.p + k, self.planes), self.t) for k in range(1, self.planes)]

    def time_others(self):
        return [(self.p, lax.rem(self.t + k, self.times)) for k in range(1, self.times)]

    def share_plane(self, blocks, send, recv):
        def start(k, carry):
            to = lax.rem(self.p + k, self.planes)
            self.copy(blocks.at[self.p], blocks.at[self.p], send.at[k], recv.at[self.p], p=to).start()
            return carry

        lax.fori_loop(1, self.planes, start, 0)

    def finish_plane(self, blocks, send, recv):
        def wait(k, carry):
            other = lax.rem(self.p + k, self.planes)
            self.copy(blocks.at[self.p], blocks.at[other], send.at[k], recv.at[other], p=other).wait()
            return carry

        lax.fori_loop(1, self.planes, wait, 0)

    def share_times(self, message, blocks, send, recv):
        def start(k, carry):
            to = lax.rem(self.t + k, self.times)
            self.copy(message, blocks.at[self.t], send.at[k], recv.at[self.t], t=to).start()
            return carry

        lax.fori_loop(1, self.times, start, 0)

    def finish_times(self, message, blocks, send, recv):
        def wait(k, carry):
            other = lax.rem(self.t + k, self.times)
            self.copy(message, blocks.at[other], send.at[k], recv.at[other], t=other).wait()
            return carry

        lax.fori_loop(1, self.times, wait, 0)


def total_of(blocks):
    total = blocks[0]
    for k in range(1, blocks.shape[0]):
        total = total + blocks[k]
    return total


def project_kernel(
    x_ref, f_ref, p_ref, g_ref,
    part, other, chip, acc, relay_in, direct_in, relay_out, joined_in,
    gram, gram_in, gram_all,
    pair_s, pair_r, ring_s, ring_r, ga_s, ga_r, gb_s, gb_r,
):
    me = Place()
    rows = acc.shape[1]
    half = rows // 2
    low, high = pl.ds(0, half), pl.ds(half, half)
    ring = me.ring
    me.greet(me.time_others() + me.plane_others())

    factors = f_ref[...]
    gram[...] = column_gram(factors, factors)
    slab = gram_in.shape[1]
    mine = gram.at[pl.ds(pl.multiple_of(me.p * slab, slab), slab)]
    me.share_times(mine, gram_in, ga_s, ga_r)
    gram_in[me.t] = mine[...]

    def block(owner):
        start = pl.multiple_of(owner * rows, rows)
        return jnp.dot(x_ref[pl.ds(start, rows), :], f_ref[...], preferred_element_type=F32)

    def to_pair(y):
        return me.copy(part.at[y], other.at[y], pair_s.at[y], pair_r.at[y], t=me.partner)

    def give(k, carry):
        y = me.ring_at(2 + 3 * k)
        part[y] = block(me.partner - me.t + me.time_of(y)).astype(BF16)
        to_pair(y).start()
        return carry

    lax.fori_loop(0, ring, give, 0)

    def chip_sum(y):
        own = block(me.time_of(y))
        to_pair(y).wait_recv()
        acc[y] = own + other[y].astype(F32)

    up, down, far = me.ring_at(1), me.ring_at(ring - 1), me.ring_at(2)
    t_up, t_down = me.time_of(up), me.time_of(down)

    chip_sum(far)
    chip[far] = acc[far].astype(BF16)
    relay_up = me.copy(chip.at[far, low], relay_in.at[0], ring_s.at[0], ring_r.at[0], t=t_up)
    relay_down = me.copy(chip.at[far, high], relay_in.at[1], ring_s.at[1], ring_r.at[1], t=t_down)
    relay_up.start()
    relay_down.start()
    chip_sum(up)
    chip[up, high] = acc[up, high].astype(BF16)
    direct_up = me.copy(chip.at[up, high], direct_in.at[0], ring_s.at[2], ring_r.at[2], t=t_up)
    direct_up.start()
    chip_sum(down)
    chip[down, low] = acc[down, low].astype(BF16)
    direct_down = me.copy(chip.at[down, low], direct_in.at[1], ring_s.at[3], ring_r.at[3], t=t_down)
    direct_down.start()

    me.finish_times(mine, gram_in, ga_s, ga_r)
    gram_all[me.p] = total_of(gram_in)
    me.share_plane(gram_all, gb_s, gb_r)

    chip_sum(me.y)

    relay_up.wait_recv()
    relay_out[0] = (acc[up, low] + relay_in[0].astype(F32)).astype(BF16)
    joined_up = me.copy(relay_out.at[0], joined_in.at[0], ring_s.at[4], ring_r.at[4], t=t_up)
    joined_up.start()
    relay_down.wait_recv()
    relay_out[1] = (acc[down, high] + relay_in[1].astype(F32)).astype(BF16)
    joined_down = me.copy(relay_out.at[1], joined_in.at[1], ring_s.at[5], ring_r.at[5], t=t_down)
    joined_down.start()

    me.finish_plane(gram_all, gb_s, gb_r)
    g_ref[...] = gram_all[...].reshape(g_ref.shape)

    direct_up.wait_recv()
    direct_down.wait_recv()
    joined_up.wait_recv()
    p_ref[low, :] = acc[me.y, low] + direct_in[1].astype(F32) + joined_in[0].astype(F32)
    joined_down.wait_recv()
    p_ref[high, :] = acc[me.y, high] + direct_in[0].astype(F32) + joined_in[1].astype(F32)

    for sent in (relay_up, relay_down, direct_up, direct_down, joined_up, joined_down):
        sent.wait_send()
    for y in range(ring):
        to_pair(y).wait_send()


def project(data, factors):
    planes, times = lax.axis_size("series"), lax.axis_size("tm")
    ring = times // 2
    n = factors.shape[1]
    rows = data.shape[0] // times
    half = rows // 2
    slab = n // planes
    return pl.pallas_call(
        project_kernel,
        out_shape=(jax.ShapeDtypeStruct((rows, n), F32), jax.ShapeDtypeStruct((n, n), F32)),
        in_specs=in_vmem(2),
        out_specs=tuple(in_vmem(2)),
        scratch_shapes=[
            pltpu.VMEM((ring, rows, n), BF16),
            pltpu.VMEM((ring, rows, n), BF16),
            pltpu.VMEM((ring, rows, n), BF16),
            pltpu.VMEM((ring, rows, n), F32),
            pltpu.VMEM((2, half, n), BF16),
            pltpu.VMEM((2, half, n), BF16),
            pltpu.VMEM((2, half, n), BF16),
            pltpu.VMEM((2, half, n), BF16),
            pltpu.VMEM((n, n), F32),
            pltpu.VMEM((times, slab, n), F32),
            pltpu.VMEM((planes, slab, n), F32),
            DMA((ring,)), DMA((ring,)), DMA((6,)), DMA((6,)),
            DMA((times,)), DMA((times,)), DMA((planes,)), DMA((planes,)),
        ],
        compiler_params=pltpu.CompilerParams(
            collective_id=0, has_side_effects=True, vmem_limit_bytes=32 * 1024 * 1024
        ),
        name="project",
    )(data, factors)


def cross_kernel(last, *refs):
    refs = list(refs)
    x_ref, l_ref, c_ref, g_ref = refs[:4]
    refs = refs[4:]
    if last:
        all_ref, square_ref = refs[:2]
        refs = refs[2:]
    lbuf, cacc, gacc, stacked, stacked_in, stacked_all = refs[:6]
    refs = refs[6:]
    pair_s, pair_r, ring_s, ring_r, ra_s, ra_r, rb_s, rb_r = refs[:8]
    me = Place()
    rows = l_ref.shape[0]
    half = rows // 2
    low, high = pl.ds(0, half), pl.ds(half, half)
    ring = me.ring
    up, down, far = me.ring_at(1), me.ring_at(ring - 1), me.ring_at(2)
    t_up, t_down, t_far = me.time_of(up), me.time_of(down), me.time_of(far)
    me.greet([(me.p, me.partner), (me.p, t_up), (me.p, t_down)] + me.plane_others())

    up_low = me.copy(l_ref.at[low], lbuf.at[me.t, low], ring_s.at[0], ring_r.at[0], t=t_up)
    down_high = me.copy(l_ref.at[high], lbuf.at[me.t, high], ring_s.at[1], ring_r.at[1], t=t_down)
    up_high = me.copy(l_ref.at[high], lbuf.at[me.t, high], ring_s.at[2], ring_r.at[2], t=t_up)
    down_low = me.copy(l_ref.at[low], lbuf.at[me.t, low], ring_s.at[3], ring_r.at[3], t=t_down)
    for sent in (up_low, down_high, up_high, down_low):
        sent.start()

    def to_pair(src, y):
        t = me.time_of(y)
        return me.copy(src, lbuf.at[t], pair_s.at[y], pair_r.at[y], t=me.partner)

    pair_own = to_pair(l_ref, me.y)
    pair_own.start()
    lbuf[me.t] = l_ref[...]
    cacc[...] = jnp.zeros_like(cacc)
    gacc[...] = jnp.zeros_like(gacc)

    def contribute(t):
        start = pl.multiple_of(t * rows, rows)
        loaded = lbuf[t]
        cacc[...] += column_gram(x_ref[pl.ds(start, rows), :], loaded)
        gacc[...] += column_gram(loaded, loaded)

    contribute(me.t)
    if last:
        def square(k, carry):
            start = pl.multiple_of(k * 64, 64)
            piece = x_ref[pl.ds(start, 64), :].astype(F32)
            piece = jnp.sum((piece * piece).reshape(8, 8, piece.shape[1]), axis=0)
            return carry + piece[:, : carry.shape[1]] + piece[:, carry.shape[1] :]

        square_ref[...] = lax.fori_loop(
            0, x_ref.shape[0] // 64, square, jnp.zeros(square_ref.shape, F32)
        )

    def across(y):
        other = me.partner - me.t + me.time_of(y)
        to_pair(lbuf.at[me.time_of(y)], y).wait_recv()
        contribute(other)

    across(me.y)
    up_low.wait_recv()
    far_up = me.copy(lbuf.at[t_down, low], lbuf.at[t_down, low], ring_s.at[4], ring_r.at[4], t=t_up)
    far_up.start()
    down_high.wait_recv()
    far_down = me.copy(lbuf.at[t_up, high], lbuf.at[t_up, high], ring_s.at[5], ring_r.at[5], t=t_down)
    far_down.start()
    up_high.wait_recv()
    pair_down = to_pair(lbuf.at[t_down], down)
    pair_down.start()
    down_low.wait_recv()
    pair_up = to_pair(lbuf.at[t_up], up)
    pair_up.start()
    contribute(t_down)
    contribute(t_up)
    across(down)
    across(up)
    far_up.wait_recv()
    far_down.wait_recv()
    pair_far = to_pair(lbuf.at[t_far], far)
    pair_far.start()
    contribute(t_far)
    across(far)

    c_slab, g_slab = c_ref.shape[0] // me.planes, g_ref.shape[0] // me.planes
    n = g_ref.shape[1]
    stacked[:, :c_slab, :] = cacc[...].reshape(me.planes, c_slab, n)
    stacked[:, c_slab:, :] = gacc[...].reshape(me.planes, g_slab, n)

    def start(k, carry):
        to = lax.rem(me.p + k, me.planes)
        me.copy(stacked.at[to], stacked_in.at[me.p], ra_s.at[k], ra_r.at[me.p], p=to).start()
        return carry

    def wait(k, carry):
        other = lax.rem(me.p + k, me.planes)
        me.copy(stacked.at[other], stacked_in.at[other], ra_s.at[k], ra_r.at[other], p=other).wait()
        return carry

    lax.fori_loop(1, me.planes, start, 0)
    if last:
        saved = pltpu.make_async_copy(lbuf, all_ref, refs[8])
        saved.start()
    stacked_in[me.p] = stacked[me.p]
    lax.fori_loop(1, me.planes, wait, 0)
    stacked_all[me.p] = total_of(stacked_in)
    me.share_plane(stacked_all, rb_s, rb_r)
    for sent in (up_low, down_high, up_high, down_low, far_up, far_down):
        sent.wait_send()
    for sent in (pair_own, pair_down, pair_up, pair_far):
        sent.wait_send()
    me.finish_plane(stacked_all, rb_s, rb_r)
    c_ref[...] = stacked_all[:, :c_slab, :].reshape(c_ref.shape)
    g_ref[...] = stacked_all[:, c_slab:, :].reshape(g_ref.shape)
    if last:
        saved.wait()


def cross_and_gram(data, share, last):
    planes, times = lax.axis_size("series"), lax.axis_size("tm")
    ring = times // 2
    rows, n = share.shape
    span = data.shape[1]
    tall = span // planes + n // planes
    out_shape = [jax.ShapeDtypeStruct((span, n), F32), jax.ShapeDtypeStruct((n, n), F32)]
    out_specs = in_vmem(2)
    extra = []
    if last:
        out_shape += [
            jax.ShapeDtypeStruct((times, rows, n), BF16),
            jax.ShapeDtypeStruct((8, n), F32),
        ]
        out_specs += [pl.BlockSpec(memory_space=pl.ANY), pl.BlockSpec(memory_space=pltpu.VMEM)]
        extra = [DMA]
    return pl.pallas_call(
        functools.partial(cross_kernel, last),
        out_shape=tuple(out_shape),
        in_specs=in_vmem(2),
        out_specs=tuple(out_specs),
        scratch_shapes=[
            pltpu.VMEM((times, rows, n), BF16),
            pltpu.VMEM((span, n), F32),
            pltpu.VMEM((n, n), F32),
            pltpu.VMEM((planes, tall, n), F32),
            pltpu.VMEM((planes, tall, n), F32),
            pltpu.VMEM((planes, tall, n), F32),
            DMA((ring,)), DMA((ring,)), DMA((6,)), DMA((6,)),
            DMA((planes,)), DMA((planes,)), DMA((planes,)), DMA((planes,)),
        ]
        + extra,
        compiler_params=pltpu.CompilerParams(
            collective_id=2 if last else 1,
            has_side_effects=True,
            vmem_limit_bytes=32 * 1024 * 1024,
        ),
        name="cross_last" if last else "cross",
    )(data, share)


def tail_kernel(
    f_ref, c_ref, gl_ref, square_ref, lag_ref, base_ref, earlier_ref, sums_ref,
    before, lag, base, message, message_in, message_all,
    row_s, row_r, ta_s, ta_r, tb_s, tb_r,
):
    me = Place()
    span, n = f_ref.shape
    edge = before.shape[0]
    me.greet(me.time_others() + me.plane_others())
    following = lax.rem(me.t + 1, me.times)
    row = me.copy(f_ref.at[pl.ds(span - edge, edge)], before, row_s, row_r, t=following)
    row.start()
    factors = f_ref[...]
    wide_factors = factors.astype(F32)
    expanded = gl_ref[...] * column_gram(factors, factors)
    fitted = -2.0 * wide_factors * c_ref[...]
    share = jnp.sum(expanded.reshape(n // 8, 8, n), axis=0)
    share = share + jnp.sum(fitted.reshape(span // 8, 8, n), axis=0)
    rolled = pltpu.roll(wide_factors, 1, 0)
    first = lax.broadcasted_iota(jnp.int32, (span, n), 0) == 0
    row.wait()
    head = before[...].astype(F32)[edge - 1 :, :]
    head = head * jnp.where(me.t == 0, 0.0, 1.0)
    earlier = jnp.where(first, head, rolled).astype(BF16)
    earlier_ref[...] = earlier
    lag[...] = column_gram(factors, earlier)
    base[...] = column_gram(earlier, earlier)
    slab = n // me.planes
    here = pl.ds(pl.multiple_of(me.p * slab, slab), slab)
    message[:slab, :] = lag[here, :]
    message[slab : 2 * slab, :] = base[here, :]
    message[2 * slab : 2 * slab + 8, :] = share
    message[2 * slab + 8 :, :] = square_ref[...]
    me.share_times(message, message_in, ta_s, ta_r)
    message_in[me.t] = message[...]
    me.finish_times(message, message_in, ta_s, ta_r)
    message_all[me.p] = total_of(message_in)
    me.share_plane(message_all, tb_s, tb_r)
    me.finish_plane(message_all, tb_s, tb_r)
    lag_ref[...] = message_all[:, :slab, :].reshape(n, n)
    base_ref[...] = message_all[:, slab : 2 * slab, :].reshape(n, n)
    sums_ref[:8, :] = message_all[0, 2 * slab : 2 * slab + 8, :]
    sums_ref[8:, :] = total_of(message_all[:, 2 * slab + 8 :, :])


def tail(factors, cross, gram_loadings, squares):
    planes, times = lax.axis_size("series"), lax.axis_size("tm")
    span, n = factors.shape
    tall = 2 * (n // planes) + 16
    square = jax.ShapeDtypeStruct((n, n), F32)
    return pl.pallas_call(
        tail_kernel,
        out_shape=(
            square,
            square,
            jax.ShapeDtypeStruct((span, n), BF16),
            jax.ShapeDtypeStruct((16, n), F32),
        ),
        in_specs=in_vmem(4),
        out_specs=tuple(in_vmem(4)),
        scratch_shapes=[
            pltpu.VMEM((16, n), BF16),
            pltpu.VMEM((n, n), F32),
            pltpu.VMEM((n, n), F32),
            pltpu.VMEM((tall, n), F32),
            pltpu.VMEM((times, tall, n), F32),
            pltpu.VMEM((planes, tall, n), F32),
            DMA, DMA, DMA((times,)), DMA((times,)), DMA((planes,)), DMA((planes,)),
        ],
        compiler_params=pltpu.CompilerParams(
            collective_id=3, has_side_effects=True, vmem_limit_bytes=32 * 1024 * 1024
        ),
        name="tail",
    )(factors, cross, gram_loadings, squares)


def fit_kernel(
    lag_ref, base_ref, f_ref, earlier_ref, sums_ref, move_ref, news_ref, share_ref, a_ref, x_ref, e_ref
):
    inverse = inverse_of(base_ref, a_ref, x_ref, e_ref)
    move = wide(lag_ref[...], inverse)
    move_ref[...] = move
    predicted = lax.dot_general(
        earlier_ref[...].astype(F32),
        move,
        (((1,), (1,)), ((), ())),
        precision=lax.Precision.HIGHEST,
        preferred_element_type=F32,
    )
    news_ref[...] = f_ref[...].astype(F32) - predicted
    total = jnp.sum(sums_ref[8:, :])
    share_ref[0, 0] = (total + jnp.sum(sums_ref[:8, :])) / total


def fit(lagged, base, factors, earlier, sums):
    span, n = factors.shape
    square = pltpu.VMEM((n, n), F32)
    return pl.pallas_call(
        fit_kernel,
        out_shape=(
            jax.ShapeDtypeStruct((n, n), F32),
            jax.ShapeDtypeStruct((span, n), F32),
            jax.ShapeDtypeStruct((1, 1), F32),
        ),
        in_specs=in_vmem(5),
        out_specs=(*in_vmem(2), pl.BlockSpec(memory_space=pltpu.SMEM)),
        scratch_shapes=[square] * 3,
        compiler_params=pltpu.CompilerParams(vmem_limit_bytes=16 * 1024 * 1024),
        name="fit",
    )(lagged, base, factors, earlier, sums)


def body(data, factors_init):
    factors = factors_init
    for sweep in range(ITERS):
        last = sweep == ITERS - 1
        projection, gram_factors = project(data, factors)
        share = solve(gram_factors, projection)
        cross, gram_loadings, *extra = cross_and_gram(data, share, last)
        factors = solve(gram_loadings, cross)
    gathered, squares = extra
    loadings = gathered.reshape(data.shape[0], factors.shape[1])
    lagged, base, earlier, sums = tail(factors, cross, gram_loadings, squares)
    transition, innovations, residual_share = fit(lagged, base, factors, earlier, sums)
    return (loadings, factors, innovations, transition, residual_share.reshape(()))


def solution(mesh):
    return jax.shard_map(
        body,
        mesh=mesh,
        in_specs=(P("series", "tm"), P("tm", None)),
        out_specs=(P("series", None), P("tm", None), P("tm", None), P(), P()),
        check_vma=False,
    )
```

```python
import functools

import jax
import jax.numpy as jnp
from jax import lax
from jax.experimental import pallas as pl
from jax.experimental.pallas import tpu as pltpu
from jax.sharding import PartitionSpec as P

ITERS = 3
RIDGE = 0.01
MESH = pl.DeviceIdType.MESH
F32 = jnp.float32
BF16 = jnp.bfloat16
DMA = pltpu.SemaphoreType.DMA


def narrow(left, right):
    return jnp.dot(left.astype(BF16), right.astype(BF16), preferred_element_type=F32)


def wide(left, right):
    return jnp.dot(left, right, precision=lax.Precision.HIGHEST, preferred_element_type=F32)


def column_gram(left, right):
    return lax.dot_general(left, right, (((0,), (0,)), ((), ())), preferred_element_type=F32)


def inverse_of(gram, a_ref, x_ref, e_ref):
    n = gram.shape[0]
    rows = lax.broadcasted_iota(jnp.int32, (n, n), 0)
    cols = lax.broadcasted_iota(jnp.int32, (n, n), 1)
    diagonal = rows == cols
    masked = jnp.where(diagonal, gram, 0.0)
    down = lax.rsqrt(jnp.sum(masked, axis=1, keepdims=True))
    across = lax.rsqrt(jnp.sum(masked, axis=0, keepdims=True))
    scaled = gram * down * across
    a_ref[...] = scaled
    bound = jnp.max(jnp.sum(jnp.abs(scaled), axis=0, keepdims=True))
    alpha = 1.9 / bound
    start = jnp.where(diagonal, alpha, 0.0)
    x_ref[...] = start
    e_ref[...] = jnp.where(diagonal, 1.0, 0.0) - alpha * scaled

    def squaring(carry):
        step, _ = carry
        for _ in range(2):
            error = e_ref[...]
            guess = x_ref[...]
            e_ref[...] = narrow(error, error)
            x_ref[...] = guess + narrow(guess, error)
        final = e_ref[...]
        return step + 1, jnp.sum(final * final)

    lax.while_loop(
        lambda c: jnp.logical_and(c[0] < 10, jnp.logical_and(c[1] > 1e-2, c[1] < 1e3)),
        squaring,
        (0, jnp.float32(1.0)),
    )

    def residual():
        error = jnp.where(diagonal, 1.0, 0.0) - wide(a_ref[...], x_ref[...])
        e_ref[...] = error
        return jnp.max(jnp.abs(error))

    def refine(carry):
        step, _ = carry
        worst = residual()
        guess = x_ref[...]
        x_ref[...] = guess + narrow(guess, e_ref[...])
        return step + 1, worst

    _, worst = lax.while_loop(
        lambda c: jnp.logical_and(c[0] < 8, jnp.logical_and(c[1] >= 5e-4, c[1] < 2.0)),
        refine,
        (0, jnp.float32(1.0)),
    )

    @pl.when(worst >= 5e-4)
    def _():
        x_ref[...] = jnp.where(diagonal, alpha, 0.0)

        def newton(carry):
            step, _ = carry
            error = residual()
            guess = x_ref[...]
            x_ref[...] = guess + wide(guess, e_ref[...])
            return step + 1, error

        lax.while_loop(
            lambda c: jnp.logical_and(c[0] < 48, c[1] >= 5e-4),
            newton,
            (0, jnp.float32(1.0)),
        )

    return x_ref[...] * down * across


class Place:
    def __init__(self):
        self.p = lax.axis_index("series")
        self.t = lax.axis_index("tm")
        self.planes = lax.axis_size("series")
        self.times = lax.axis_size("tm")
        self.ring = self.times // 2
        self.y = lax.div(self.t, 2)
        self.c = lax.rem(self.t, 2)
        self.partner = self.t + 1 - 2 * self.c

    def ring_at(self, distance):
        return lax.rem(self.y + distance, self.ring)

    def time_of(self, y):
        return 2 * y + self.c

    def copy(self, src, dst, send, recv, p=None, t=None):
        return pltpu.make_async_remote_copy(
            src_ref=src,
            dst_ref=dst,
            send_sem=send,
            recv_sem=recv,
            device_id=(self.p if p is None else p, self.t if t is None else t),
            device_id_type=MESH,
        )

    def greet(self, others):
        barrier = pltpu.get_barrier_semaphore()
        for p, t in others:
            pl.semaphore_signal(barrier, inc=1, device_id=(p, t), device_id_type=MESH)
        pl.semaphore_wait(barrier, len(others))

    def plane_others(self):
        return [(lax.rem(self.p + k, self.planes), self.t) for k in range(1, self.planes)]

    def time_others(self):
        return [(self.p, lax.rem(self.t + k, self.times)) for k in range(1, self.times)]

    def share_plane(self, message, blocks, send, recv):
        def start(k, carry):
            to = lax.rem(self.p + k, self.planes)
            self.copy(message, blocks.at[self.p], send.at[k], recv.at[self.p], p=to).start()
            return carry

        lax.fori_loop(1, self.planes, start, 0)

    def finish_plane(self, message, blocks, send, recv):
        def wait(k, carry):
            other = lax.rem(self.p + k, self.planes)
            self.copy(message, blocks.at[other], send.at[k], recv.at[other], p=other).wait()
            return carry

        lax.fori_loop(1, self.planes, wait, 0)

    def spread_plane(self, pieces, blocks, send, recv):
        def start(k, carry):
            to = lax.rem(self.p + k, self.planes)
            self.copy(pieces.at[to], blocks.at[self.p], send.at[k], recv.at[self.p], p=to).start()
            return carry

        lax.fori_loop(1, self.planes, start, 0)

    def finish_spread(self, pieces, blocks, send, recv):
        def wait(k, carry):
            other = lax.rem(self.p + k, self.planes)
            self.copy(pieces.at[other], blocks.at[other], send.at[k], recv.at[other], p=other).wait()
            return carry

        lax.fori_loop(1, self.planes, wait, 0)

    def share_times(self, message, blocks, send, recv):
        def start(k, carry):
            to = lax.rem(self.t + k, self.times)
            self.copy(message, blocks.at[self.t], send.at[k], recv.at[self.t], t=to).start()
            return carry

        lax.fori_loop(1, self.times, start, 0)

    def finish_times(self, message, blocks, send, recv):
        def wait(k, carry):
            other = lax.rem(self.t + k, self.times)
            self.copy(message, blocks.at[other], send.at[k], recv.at[other], t=other).wait()
            return carry

        lax.fori_loop(1, self.times, wait, 0)


def total_of(blocks):
    total = blocks[0]
    for k in range(1, blocks.shape[0]):
        total = total + blocks[k]
    return total


def in_vmem(count):
    return [pl.BlockSpec(memory_space=pltpu.VMEM)] * count


def sweep_kernel(first, last, *refs):
    refs = list(refs)

    def take(count):
        taken, refs[:] = refs[:count], refs[count:]
        return taken

    x_ref, f_ref, w_ref, m_ref, g_ref = take(5)
    if last:
        all_ref, square_ref = take(2)
    if not first:
        fbuf, f_s, f_r = take(3)
    part, other, chip, acc, relay_in, direct_in, relay_out, joined_in = take(8)
    gram, gram_in, gram_all, moment, moment_in, moment_own, moment_times, moment_all = take(8)
    pbuf, wacc, winc = take(3)
    pair_s, pair_r, ring_s, ring_r, ga_s, ga_r, gb_s, gb_r = take(8)
    gpair_s, gpair_r, gring_s, gring_r, ma_s, ma_r, mb_s, mb_r, mc_s, mc_r, w_s, w_r = take(12)
    me = Place()
    rows = acc.shape[1]
    half = rows // 2
    low, high = pl.ds(0, half), pl.ds(half, half)
    ring = me.ring
    up, down, far = me.ring_at(1), me.ring_at(ring - 1), me.ring_at(2)
    t_up, t_down, t_far = me.time_of(up), me.time_of(down), me.time_of(far)
    slab = gram_in.shape[1]
    me.greet(me.time_others() + me.plane_others())

    if first:
        def factors():
            return f_ref[...]
    else:
        me.share_plane(f_ref, fbuf, f_s, f_r)
        fbuf[me.p] = f_ref[...]
        me.finish_plane(f_ref, fbuf, f_s, f_r)

        def factors():
            return fbuf[...].reshape(x_ref.shape[1], f_ref.shape[1])

    gram[...] = column_gram(factors(), factors())
    mine = gram.at[pl.ds(pl.multiple_of(me.p * slab, slab), slab)]
    me.share_times(mine, gram_in, ga_s, ga_r)
    gram_in[me.t] = mine[...]

    def block(owner):
        start = pl.multiple_of(owner * rows, rows)
        return jnp.dot(x_ref[pl.ds(start, rows), :], factors(), preferred_element_type=F32)

    def to_pair(y):
        return me.copy(part.at[y], other.at[y], pair_s.at[y], pair_r.at[y], t=me.partner)

    def give(k, carry):
        y = me.ring_at(2 + 3 * k)
        part[y] = block(me.partner - me.t + me.time_of(y)).astype(BF16)
        to_pair(y).start()
        return carry

    lax.fori_loop(0, ring, give, 0)

    def chip_sum(y):
        own = block(me.time_of(y))
        to_pair(y).wait_recv()
        acc[y] = own + other[y].astype(F32)

    chip_sum(far)
    chip[far] = acc[far].astype(BF16)
    relay_up = me.copy(chip.at[far, low], relay_in.at[0], ring_s.at[0], ring_r.at[0], t=t_up)
    relay_down = me.copy(chip.at[far, high], relay_in.at[1], ring_s.at[1], ring_r.at[1], t=t_down)
    relay_up.start()
    relay_down.start()
    chip_sum(up)
    chip[up, high] = acc[up, high].astype(BF16)
    direct_up = me.copy(chip.at[up, high], direct_in.at[0], ring_s.at[2], ring_r.at[2], t=t_up)
    direct_up.start()
    chip_sum(down)
    chip[down, low] = acc[down, low].astype(BF16)
    direct_down = me.copy(chip.at[down, low], direct_in.at[1], ring_s.at[3], ring_r.at[3], t=t_down)
    direct_down.start()
    chip_sum(me.y)

    relay_up.wait_recv()
    relay_out[0] = (acc[up, low] + relay_in[0].astype(F32)).astype(BF16)
    joined_up = me.copy(relay_out.at[0], joined_in.at[0], ring_s.at[4], ring_r.at[4], t=t_up)
    joined_up.start()
    relay_down.wait_recv()
    relay_out[1] = (acc[down, high] + relay_in[1].astype(F32)).astype(BF16)
    joined_down = me.copy(relay_out.at[1], joined_in.at[1], ring_s.at[5], ring_r.at[5], t=t_down)
    joined_down.start()

    me.finish_times(mine, gram_in, ga_s, ga_r)
    gram_all[me.p] = total_of(gram_in)
    me.share_plane(gram_all.at[me.p], gram_all, gb_s, gb_r)

    direct_up.wait_recv()
    direct_down.wait_recv()
    joined_up.wait_recv()
    pbuf[me.t, low] = (
        acc[me.y, low] + direct_in[1].astype(F32) + joined_in[0].astype(F32)
    ).astype(BF16)
    mine_low, mine_high = pbuf.at[me.t, low], pbuf.at[me.t, high]
    up_low = me.copy(mine_low, mine_low, gring_s.at[0], gring_r.at[0], t=t_up)
    up_low.start()
    joined_down.wait_recv()
    pbuf[me.t, high] = (
        acc[me.y, high] + direct_in[0].astype(F32) + joined_in[1].astype(F32)
    ).astype(BF16)
    down_high = me.copy(mine_high, mine_high, gring_s.at[1], gring_r.at[1], t=t_down)
    down_high.start()
    up_high = me.copy(mine_high, mine_high, gring_s.at[2], gring_r.at[2], t=t_up)
    up_high.start()
    down_low = me.copy(mine_low, mine_low, gring_s.at[3], gring_r.at[3], t=t_down)
    down_low.start()

    def pass_over(y):
        piece = pbuf.at[me.time_of(y)]
        return me.copy(piece, piece, gpair_s.at[y], gpair_r.at[y], t=me.partner)

    pass_over(me.y).start()

    own_rows = pbuf[me.t]
    moment[...] = column_gram(own_rows, own_rows).reshape(moment.shape)
    me.spread_plane(moment, moment_in, ma_s, ma_r)
    moment_in[me.p] = moment[me.p]

    wacc[...] = jnp.zeros_like(wacc)

    def contribute(t):
        start = pl.multiple_of(t * rows, rows)
        wacc[...] += column_gram(x_ref[pl.ds(start, rows), :], pbuf[t]).reshape(wacc.shape)

    def across(y):
        pass_over(y).wait_recv()
        contribute(me.partner - me.t + me.time_of(y))

    contribute(me.t)
    across(me.y)
    if last:
        def square(k, carry):
            start = pl.multiple_of(k * 64, 64)
            piece = x_ref[pl.ds(start, 64), :].astype(F32)
            piece = jnp.sum((piece * piece).reshape(8, 8, piece.shape[1]), axis=0)
            return carry + piece[:, : carry.shape[1]] + piece[:, carry.shape[1] :]

        square_ref[...] = lax.fori_loop(
            0, x_ref.shape[0] // 64, square, jnp.zeros(square_ref.shape, F32)
        )
    up_low.wait_recv()
    far_low = pbuf.at[t_down, low]
    far_up = me.copy(far_low, far_low, gring_s.at[4], gring_r.at[4], t=t_up)
    far_up.start()
    down_high.wait_recv()
    far_high = pbuf.at[t_up, high]
    far_down = me.copy(far_high, far_high, gring_s.at[5], gring_r.at[5], t=t_down)
    far_down.start()

    me.finish_spread(moment, moment_in, ma_s, ma_r)
    moment_own[...] = total_of(moment_in)
    me.share_times(moment_own, moment_times, mb_s, mb_r)
    moment_times[me.t] = moment_own[...]

    up_high.wait_recv()
    pass_over(down).start()
    down_low.wait_recv()
    pass_over(up).start()
    contribute(t_down)
    contribute(t_up)
    across(down)
    across(up)
    me.finish_times(moment_own, moment_times, mb_s, mb_r)
    moment_all[me.p] = total_of(moment_times)
    me.share_plane(moment_all.at[me.p], moment_all, mc_s, mc_r)
    far_up.wait_recv()
    far_down.wait_recv()
    pass_over(far).start()
    contribute(t_far)
    across(far)

    me.spread_plane(wacc, winc, w_s, w_r)
    winc[me.p] = wacc[me.p]
    if last:
        all_ref[...] = pbuf[...]
    me.finish_plane(gram_all.at[me.p], gram_all, gb_s, gb_r)
    g_ref[...] = gram_all[...].reshape(g_ref.shape)
    me.finish_plane(moment_all.at[me.p], moment_all, mc_s, mc_r)
    m_ref[...] = moment_all[...].reshape(m_ref.shape)
    me.finish_spread(wacc, winc, w_s, w_r)
    w_ref[...] = total_of(winc)

    for sent in (relay_up, relay_down, direct_up, direct_down, joined_up, joined_down):
        sent.wait_send()
    for sent in (up_low, down_high, up_high, down_low, far_up, far_down):
        sent.wait_send()
    for y in range(ring):
        to_pair(y).wait_send()
        pass_over(y).wait_send()


def sweep(data, factors, first, last):
    planes, times = lax.axis_size("series"), lax.axis_size("tm")
    ring = times // 2
    n = factors.shape[1]
    span = data.shape[1]
    rows = data.shape[0] // times
    half = rows // 2
    slab, tall = n // planes, span // planes
    out_shape = [
        jax.ShapeDtypeStruct((tall, n), F32),
        jax.ShapeDtypeStruct((n, n), F32),
        jax.ShapeDtypeStruct((n, n), F32),
    ]
    if last:
        out_shape += [
            jax.ShapeDtypeStruct((times, rows, n), BF16),
            jax.ShapeDtypeStruct((8, n), F32),
        ]
    scratch = []
    if not first:
        scratch += [pltpu.VMEM((planes, tall, n), BF16), DMA((planes,)), DMA((planes,))]
    scratch += [pltpu.VMEM((ring, rows, n), BF16)] * 3 + [pltpu.VMEM((ring, rows, n), F32)]
    scratch += [pltpu.VMEM((2, half, n), BF16)] * 4
    scratch += [
        pltpu.VMEM((n, n), F32),
        pltpu.VMEM((times, slab, n), F32),
        pltpu.VMEM((planes, slab, n), F32),
        pltpu.VMEM((planes, slab, n), F32),
        pltpu.VMEM((planes, slab, n), F32),
        pltpu.VMEM((slab, n), F32),
        pltpu.VMEM((times, slab, n), F32),
        pltpu.VMEM((planes, slab, n), F32),
        pltpu.VMEM((times, rows, n), BF16),
        pltpu.VMEM((planes, tall, n), F32),
        pltpu.VMEM((planes, tall, n), F32),
    ]
    scratch += [DMA((ring,)), DMA((ring,)), DMA((6,)), DMA((6,))]
    scratch += [DMA((times,)), DMA((times,)), DMA((planes,)), DMA((planes,))]
    scratch += [DMA((ring,)), DMA((ring,)), DMA((6,)), DMA((6,))]
    scratch += [DMA((planes,)), DMA((planes,)), DMA((times,)), DMA((times,))]
    scratch += [DMA((planes,)), DMA((planes,)), DMA((planes,)), DMA((planes,))]
    return pl.pallas_call(
        functools.partial(sweep_kernel, first, last),
        out_shape=tuple(out_shape),
        in_specs=in_vmem(2),
        out_specs=tuple(in_vmem(len(out_shape))),
        scratch_shapes=scratch,
        compiler_params=pltpu.CompilerParams(
            collective_id=0 if first else 2 if last else 1,
            has_side_effects=True,
            vmem_limit_bytes=32 * 1024 * 1024,
        ),
        name="sweep_first" if first else "sweep_last" if last else "sweep",
    )(data, factors)


def regularized(gram):
    shape = gram.shape
    diagonal = lax.broadcasted_iota(jnp.int32, shape, 0) == lax.broadcasted_iota(jnp.int32, shape, 1)
    return gram + jnp.where(diagonal, RIDGE, 0.0)


def next_factors(w_ref, m_ref, ridged, a_ref, x_ref, e_ref):
    combined = m_ref[...] + RIDGE * wide(ridged, ridged)
    inverse = inverse_of(combined, a_ref, x_ref, e_ref)
    return wide(wide(w_ref[...], inverse), ridged).astype(BF16)


def solve_kernel(w_ref, m_ref, g_ref, f_ref, a_ref, x_ref, e_ref):
    f_ref[...] = next_factors(w_ref, m_ref, regularized(g_ref[...]), a_ref, x_ref, e_ref)


def solve(cross, moment, gram):
    square = pltpu.VMEM(gram.shape, F32)
    return pl.pallas_call(
        solve_kernel,
        out_shape=jax.ShapeDtypeStruct(cross.shape, BF16),
        in_specs=in_vmem(3),
        out_specs=in_vmem(1)[0],
        scratch_shapes=[square] * 3,
        compiler_params=pltpu.CompilerParams(vmem_limit_bytes=16 * 1024 * 1024),
        name="solve",
    )(cross, moment, gram)


def folded(rows):
    rows = jnp.sum(rows.reshape(rows.shape[0] // 8, 8, rows.shape[1]), axis=0)
    side = rows.shape[1] // 2
    return rows[:, :side] + rows[:, side:]


def solve_last_kernel(
    w_ref, m_ref, g_ref, p_ref, square_ref, f_ref, l_ref, sums_ref, a_ref, x_ref, e_ref
):
    ridged = regularized(g_ref[...])
    factors = next_factors(w_ref, m_ref, ridged, a_ref, x_ref, e_ref)
    f_ref[...] = factors
    inverse = inverse_of(ridged, a_ref, x_ref, e_ref)
    top = inverse.astype(BF16)
    rest = inverse - top.astype(F32)
    middle = rest.astype(BF16)
    bottom = (rest - middle.astype(F32)).astype(BF16)

    def load(k, carry):
        rows = p_ref[k]
        l_ref[k] = (narrow(rows, bottom) + narrow(rows, middle) + narrow(rows, top)).astype(BF16)
        return carry

    lax.fori_loop(0, p_ref.shape[0], load, 0)
    known = factors.astype(F32)
    quadratic = wide(wide(inverse, m_ref[...]), inverse)
    side = sums_ref.shape[1] // 2
    sums_ref[:, :side] = folded(wide(known, quadratic) * known) - 2.0 * folded(
        wide(known, inverse) * w_ref[...]
    )
    sums_ref[:, side:] = folded(square_ref[...])


def solve_last(cross, moment, gram, projection, squares):
    square = pltpu.VMEM(gram.shape, F32)
    return pl.pallas_call(
        solve_last_kernel,
        out_shape=(
            jax.ShapeDtypeStruct(cross.shape, BF16),
            jax.ShapeDtypeStruct(projection.shape, BF16),
            jax.ShapeDtypeStruct(squares.shape, F32),
        ),
        in_specs=in_vmem(5),
        out_specs=tuple(in_vmem(3)),
        scratch_shapes=[square] * 3,
        compiler_params=pltpu.CompilerParams(vmem_limit_bytes=16 * 1024 * 1024),
        name="solve_last",
    )(cross, moment, gram, projection, squares)


def tail_kernel(
    f_ref, own_ref, all_ref, lag_ref, base_ref, earlier_ref, sums_ref,
    fbuf, before, lag, base, message, message_in, message_all,
    f_s, f_r, row_s, row_r, ta_s, ta_r, tb_s, tb_r,
):
    me = Place()
    span, n = all_ref.shape
    edge = before.shape[0]
    me.greet(me.time_others() + me.plane_others())
    me.share_plane(f_ref, fbuf, f_s, f_r)
    fbuf[me.p] = f_ref[...]
    me.finish_plane(f_ref, fbuf, f_s, f_r)
    following = lax.rem(me.t + 1, me.times)
    last_rows = fbuf.at[me.planes - 1, pl.ds(fbuf.shape[1] - edge, edge)]
    row = me.copy(last_rows, before, row_s, row_r, t=following)
    row.start()
    factors = fbuf[...].reshape(span, n)
    all_ref[...] = factors
    rolled = pltpu.roll(factors.astype(F32), 1, 0)
    first = lax.broadcasted_iota(jnp.int32, (span, n), 0) == 0
    row.wait()
    head = before[...].astype(F32)[edge - 1 :, :]
    head = head * jnp.where(me.t == 0, 0.0, 1.0)
    earlier = jnp.where(first, head, rolled).astype(BF16)
    earlier_ref[...] = earlier
    lag[...] = column_gram(factors, earlier)
    base[...] = column_gram(earlier, earlier)
    slab = n // me.planes
    here = pl.ds(pl.multiple_of(me.p * slab, slab), slab)
    message[:slab, :] = lag[here, :]
    message[slab : 2 * slab, :] = base[here, :]
    message[2 * slab :, :] = own_ref[...]
    me.share_times(message, message_in, ta_s, ta_r)
    message_in[me.t] = message[...]
    me.finish_times(message, message_in, ta_s, ta_r)
    message_all[me.p] = total_of(message_in)
    me.share_plane(message_all.at[me.p], message_all, tb_s, tb_r)
    me.finish_plane(message_all.at[me.p], message_all, tb_s, tb_r)
    lag_ref[...] = message_all[:, :slab, :].reshape(n, n)
    base_ref[...] = message_all[:, slab : 2 * slab, :].reshape(n, n)
    sums_ref[...] = total_of(message_all[:, 2 * slab :, :])


def tail(factors, own):
    planes, times = lax.axis_size("series"), lax.axis_size("tm")
    slab, n = factors.shape
    span = slab * planes
    tall = 2 * (n // planes) + own.shape[0]
    square = jax.ShapeDtypeStruct((n, n), F32)
    block = jax.ShapeDtypeStruct((span, n), BF16)
    return pl.pallas_call(
        tail_kernel,
        out_shape=(block, square, square, block, jax.ShapeDtypeStruct(own.shape, F32)),
        in_specs=in_vmem(2),
        out_specs=tuple(in_vmem(5)),
        scratch_shapes=[
            pltpu.VMEM((planes, slab, n), BF16),
            pltpu.VMEM((16, n), BF16),
            pltpu.VMEM((n, n), F32),
            pltpu.VMEM((n, n), F32),
            pltpu.VMEM((tall, n), F32),
            pltpu.VMEM((times, tall, n), F32),
            pltpu.VMEM((planes, tall, n), F32),
            DMA((planes,)), DMA((planes,)), DMA, DMA,
            DMA((times,)), DMA((times,)), DMA((planes,)), DMA((planes,)),
        ],
        compiler_params=pltpu.CompilerParams(
            collective_id=3, has_side_effects=True, vmem_limit_bytes=32 * 1024 * 1024
        ),
        name="tail",
    )(factors, own)


def fit_kernel(
    lag_ref, base_ref, f_ref, earlier_ref, sums_ref,
    move_ref, news_ref, factors_ref, share_ref, a_ref, x_ref, e_ref,
):
    inverse = inverse_of(regularized(base_ref[...]), a_ref, x_ref, e_ref)
    move = wide(lag_ref[...], inverse)
    move_ref[...] = move
    predicted = lax.dot_general(
        earlier_ref[...].astype(F32),
        move,
        (((1,), (1,)), ((), ())),
        precision=lax.Precision.HIGHEST,
        preferred_element_type=F32,
    )
    news_ref[...] = f_ref[...].astype(F32) - predicted
    factors_ref[...] = f_ref[...]
    side = sums_ref.shape[1] // 2
    total = jnp.sum(sums_ref[:, side:])
    share_ref[0, 0] = (total + jnp.sum(sums_ref[:, :side])) / total


def fit(lagged, base, factors, earlier, sums):
    span, n = factors.shape
    square = pltpu.VMEM((n, n), F32)
    return pl.pallas_call(
        fit_kernel,
        out_shape=(
            jax.ShapeDtypeStruct((n, n), F32),
            jax.ShapeDtypeStruct((span, n), F32),
            jax.ShapeDtypeStruct((span, n), BF16),
            jax.ShapeDtypeStruct((1, 1), F32),
        ),
        in_specs=in_vmem(5),
        out_specs=(*in_vmem(3), pl.BlockSpec(memory_space=pltpu.SMEM)),
        scratch_shapes=[square] * 3,
        compiler_params=pltpu.CompilerParams(vmem_limit_bytes=16 * 1024 * 1024),
        name="fit",
    )(lagged, base, factors, earlier, sums)


def body(data, factors_init):
    factors = factors_init
    for step in range(ITERS):
        first, last = step == 0, step == ITERS - 1
        cross, moment, gram, *extra = sweep(data, factors, first, last)
        if not last:
            factors = solve(cross, moment, gram)
    projection, squares = extra
    factors, loadings, own = solve_last(cross, moment, gram, projection, squares)
    loadings = loadings.reshape(data.shape[0], factors.shape[1])
    gathered, lagged, base, earlier, sums = tail(factors, own)
    transition, innovations, factors, share = fit(lagged, base, gathered, earlier, sums)
    return (loadings, factors, innovations, transition, share.reshape(()))


def solution(mesh):
    return jax.shard_map(
        body,
        mesh=mesh,
        in_specs=(P("series", "tm"), P("tm", None)),
        out_specs=(P("series", None), P("tm", None), P("tm", None), P(), P()),
        check_vma=False,
    )
```

```python
import functools

import jax
import jax.numpy as jnp
from jax import lax
from jax.experimental import pallas as pl
from jax.experimental.pallas import tpu as pltpu
from jax.sharding import PartitionSpec as P

ITERS = 3
RIDGE = 0.01
MESH = pl.DeviceIdType.MESH
F32 = jnp.float32
BF16 = jnp.bfloat16
DMA = pltpu.SemaphoreType.DMA


def narrow(left, right):
    return jnp.dot(left.astype(BF16), right.astype(BF16), preferred_element_type=F32)


def wide(left, right):
    return jnp.dot(left, right, precision=lax.Precision.HIGHEST, preferred_element_type=F32)


def column_gram(left, right):
    return lax.dot_general(left, right, (((0,), (0,)), ((), ())), preferred_element_type=F32)


def inverses_of(grams, a_ref, x_ref, e_ref):
    n = grams[0].shape[0]
    each = range(len(grams))
    rows = lax.broadcasted_iota(jnp.int32, (n, n), 0)
    cols = lax.broadcasted_iota(jnp.int32, (n, n), 1)
    diagonal = rows == cols
    down, across, alpha = [], [], []
    for i in each:
        masked = jnp.where(diagonal, grams[i], 0.0)
        down.append(lax.rsqrt(jnp.sum(masked, axis=1, keepdims=True)))
        across.append(lax.rsqrt(jnp.sum(masked, axis=0, keepdims=True)))
        scaled = grams[i] * down[i] * across[i]
        a_ref[i] = scaled
        alpha.append(1.9 / jnp.max(jnp.sum(jnp.abs(scaled), axis=0, keepdims=True)))
        x_ref[i] = jnp.where(diagonal, alpha[i], 0.0)
        e_ref[i] = jnp.where(diagonal, 1.0, 0.0) - alpha[i] * scaled

    def worst_of(values):
        return functools.reduce(jnp.maximum, values)

    def squaring(carry):
        step, _ = carry
        for _ in range(2):
            for i in each:
                error = e_ref[i]
                guess = x_ref[i]
                e_ref[i] = narrow(error, error)
                x_ref[i] = guess + narrow(guess, error)
        return step + 1, worst_of([jnp.sum(e_ref[i] * e_ref[i]) for i in each])

    lax.while_loop(
        lambda c: jnp.logical_and(c[0] < 10, jnp.logical_and(c[1] > 1e-2, c[1] < 1e3)),
        squaring,
        (0, jnp.float32(1.0)),
    )

    def residual():
        for i in each:
            e_ref[i] = jnp.where(diagonal, 1.0, 0.0) - wide(a_ref[i], x_ref[i])
        return worst_of([jnp.max(jnp.abs(e_ref[i])) for i in each])

    def refine(carry):
        step, _ = carry
        worst = residual()
        for i in each:
            guess = x_ref[i]
            x_ref[i] = guess + narrow(guess, e_ref[i])
        return step + 1, worst

    _, worst = lax.while_loop(
        lambda c: jnp.logical_and(c[0] < 8, jnp.logical_and(c[1] >= 5e-4, c[1] < 2.0)),
        refine,
        (0, jnp.float32(1.0)),
    )

    @pl.when(worst >= 5e-4)
    def _():
        for i in each:
            x_ref[i] = jnp.where(diagonal, alpha[i], 0.0)

        def newton(carry):
            step, _ = carry
            error = residual()
            for i in each:
                guess = x_ref[i]
                x_ref[i] = guess + wide(guess, e_ref[i])
            return step + 1, error

        lax.while_loop(
            lambda c: jnp.logical_and(c[0] < 48, c[1] >= 5e-4),
            newton,
            (0, jnp.float32(1.0)),
        )

    return [x_ref[i] * down[i] * across[i] for i in each]


def squares_of(count, n):
    return [pltpu.VMEM((count, n, n), F32)] * 3


class Place:
    def __init__(self):
        self.p = lax.axis_index("series")
        self.t = lax.axis_index("tm")
        self.planes = lax.axis_size("series")
        self.times = lax.axis_size("tm")
        self.ring = self.times // 2
        self.y = lax.div(self.t, 2)
        self.c = lax.rem(self.t, 2)
        self.partner = self.t + 1 - 2 * self.c

    def ring_at(self, distance):
        return lax.rem(self.y + distance, self.ring)

    def time_of(self, y):
        return 2 * y + self.c

    def copy(self, src, dst, send, recv, p=None, t=None):
        return pltpu.make_async_remote_copy(
            src_ref=src,
            dst_ref=dst,
            send_sem=send,
            recv_sem=recv,
            device_id=(self.p if p is None else p, self.t if t is None else t),
            device_id_type=MESH,
        )

    def greet(self, others, meanwhile=None):
        barrier = pltpu.get_barrier_semaphore()
        for p, t in others:
            pl.semaphore_signal(barrier, inc=1, device_id=(p, t), device_id_type=MESH)
        if meanwhile is not None:
            meanwhile()
        pl.semaphore_wait(barrier, len(others))

    def plane_others(self):
        return [(lax.rem(self.p + k, self.planes), self.t) for k in range(1, self.planes)]

    def time_others(self):
        return [(self.p, lax.rem(self.t + k, self.times)) for k in range(1, self.times)]

    def share_plane(self, message, blocks, send, recv):
        def start(k, carry):
            to = lax.rem(self.p + k, self.planes)
            self.copy(message, blocks.at[self.p], send.at[k], recv.at[self.p], p=to).start()
            return carry

        lax.fori_loop(1, self.planes, start, 0)

    def finish_plane(self, message, blocks, send, recv):
        def wait(k, carry):
            other = lax.rem(self.p + k, self.planes)
            self.copy(message, blocks.at[other], send.at[k], recv.at[other], p=other).wait()
            return carry

        lax.fori_loop(1, self.planes, wait, 0)

    def spread_plane(self, pieces, blocks, send, recv):
        def start(k, carry):
            to = lax.rem(self.p + k, self.planes)
            self.copy(pieces.at[to], blocks.at[self.p], send.at[k], recv.at[self.p], p=to).start()
            return carry

        lax.fori_loop(1, self.planes, start, 0)

    def finish_spread(self, pieces, blocks, send, recv):
        def wait(k, carry):
            other = lax.rem(self.p + k, self.planes)
            self.copy(pieces.at[other], blocks.at[other], send.at[k], recv.at[other], p=other).wait()
            return carry

        lax.fori_loop(1, self.planes, wait, 0)

    def share_times(self, message, blocks, send, recv):
        def start(k, carry):
            to = lax.rem(self.t + k, self.times)
            self.copy(message, blocks.at[self.t], send.at[k], recv.at[self.t], t=to).start()
            return carry

        lax.fori_loop(1, self.times, start, 0)

    def finish_times(self, message, blocks, send, recv):
        def wait(k, carry):
            other = lax.rem(self.t + k, self.times)
            self.copy(message, blocks.at[other], send.at[k], recv.at[other], t=other).wait()
            return carry

        lax.fori_loop(1, self.times, wait, 0)


def total_of(blocks):
    total = blocks[0]
    for k in range(1, blocks.shape[0]):
        total = total + blocks[k]
    return total


def in_vmem(count):
    return [pl.BlockSpec(memory_space=pltpu.VMEM)] * count


def sweep_kernel(first, last, *refs):
    refs = list(refs)

    def take(count):
        taken, refs[:] = refs[:count], refs[count:]
        return taken

    x_ref, f_ref, w_ref, m_ref, g_ref = take(5)
    if last:
        all_ref, square_ref = take(2)
    if first:
        x_from = x_ref
        x_ref, x_sem = take(2)
    else:
        fbuf, f_s, f_r = take(3)
    part, other, chip, acc, relay_in, direct_in, relay_out, joined_in = take(8)
    gram, gram_in, gram_all, moment, moment_in, moment_own, moment_times, moment_all = take(8)
    pbuf, wacc, winc = take(3)
    pair_s, pair_r, ring_s, ring_r, ga_s, ga_r, gb_s, gb_r = take(8)
    gpair_s, gpair_r, gring_s, gring_r, ma_s, ma_r, mb_s, mb_r, mc_s, mc_r, w_s, w_r = take(12)
    me = Place()
    rows = acc.shape[1]
    half = rows // 2
    low, high = pl.ds(0, half), pl.ds(half, half)
    ring = me.ring
    up, down, far = me.ring_at(1), me.ring_at(ring - 1), me.ring_at(2)
    t_up, t_down, t_far = me.time_of(up), me.time_of(down), me.time_of(far)
    slab = gram_in.shape[1]

    def bring():
        x_copy = pltpu.make_async_copy(x_from, x_ref, x_sem)
        x_copy.start()
        gram[...] = column_gram(f_ref[...], f_ref[...])
        x_copy.wait()

    me.greet(me.time_others() + me.plane_others(), bring if first else None)

    if first:
        def factors():
            return f_ref[...]
    else:
        me.share_plane(f_ref, fbuf, f_s, f_r)
        fbuf[me.p] = f_ref[...]
        me.finish_plane(f_ref, fbuf, f_s, f_r)

        def factors():
            return fbuf[...].reshape(x_ref.shape[1], f_ref.shape[1])

    if not first:
        gram[...] = column_gram(factors(), factors())
    mine = gram.at[pl.ds(pl.multiple_of(me.p * slab, slab), slab)]
    me.share_times(mine, gram_in, ga_s, ga_r)
    gram_in[me.t] = mine[...]

    def block(owner):
        start = pl.multiple_of(owner * rows, rows)
        return jnp.dot(x_ref[pl.ds(start, rows), :], factors(), preferred_element_type=F32)

    def to_pair(y):
        return me.copy(part.at[y], other.at[y], pair_s.at[y], pair_r.at[y], t=me.partner)

    def give(k, carry):
        y = me.ring_at(2 + 3 * k)
        part[y] = block(me.partner - me.t + me.time_of(y)).astype(BF16)
        to_pair(y).start()
        return carry

    lax.fori_loop(0, ring, give, 0)

    def chip_sum(y):
        own = block(me.time_of(y))
        to_pair(y).wait_recv()
        acc[y] = own + other[y].astype(F32)

    chip_sum(far)
    chip[far] = acc[far].astype(BF16)
    relay_up = me.copy(chip.at[far, low], relay_in.at[0], ring_s.at[0], ring_r.at[0], t=t_up)
    relay_down = me.copy(chip.at[far, high], relay_in.at[1], ring_s.at[1], ring_r.at[1], t=t_down)
    relay_up.start()
    relay_down.start()
    chip_sum(up)
    chip[up, high] = acc[up, high].astype(BF16)
    direct_up = me.copy(chip.at[up, high], direct_in.at[0], ring_s.at[2], ring_r.at[2], t=t_up)
    direct_up.start()
    chip_sum(down)
    chip[down, low] = acc[down, low].astype(BF16)
    direct_down = me.copy(chip.at[down, low], direct_in.at[1], ring_s.at[3], ring_r.at[3], t=t_down)
    direct_down.start()
    chip_sum(me.y)

    relay_up.wait_recv()
    relay_out[0] = (acc[up, low] + relay_in[0].astype(F32)).astype(BF16)
    joined_up = me.copy(relay_out.at[0], joined_in.at[0], ring_s.at[4], ring_r.at[4], t=t_up)
    joined_up.start()
    relay_down.wait_recv()
    relay_out[1] = (acc[down, high] + relay_in[1].astype(F32)).astype(BF16)
    joined_down = me.copy(relay_out.at[1], joined_in.at[1], ring_s.at[5], ring_r.at[5], t=t_down)
    joined_down.start()

    me.finish_times(mine, gram_in, ga_s, ga_r)
    gram_all[me.p] = total_of(gram_in)
    me.share_plane(gram_all.at[me.p], gram_all, gb_s, gb_r)

    direct_up.wait_recv()
    direct_down.wait_recv()
    joined_up.wait_recv()
    pbuf[me.t, low] = (
        acc[me.y, low] + direct_in[1].astype(F32) + joined_in[0].astype(F32)
    ).astype(BF16)
    mine_low, mine_high = pbuf.at[me.t, low], pbuf.at[me.t, high]
    up_low = me.copy(mine_low, mine_low, gring_s.at[0], gring_r.at[0], t=t_up)
    up_low.start()
    joined_down.wait_recv()
    pbuf[me.t, high] = (
        acc[me.y, high] + direct_in[0].astype(F32) + joined_in[1].astype(F32)
    ).astype(BF16)
    down_high = me.copy(mine_high, mine_high, gring_s.at[1], gring_r.at[1], t=t_down)
    down_high.start()
    up_high = me.copy(mine_high, mine_high, gring_s.at[2], gring_r.at[2], t=t_up)
    up_high.start()
    down_low = me.copy(mine_low, mine_low, gring_s.at[3], gring_r.at[3], t=t_down)
    down_low.start()

    def pass_over(y):
        piece = pbuf.at[me.time_of(y)]
        return me.copy(piece, piece, gpair_s.at[y], gpair_r.at[y], t=me.partner)

    pass_over(me.y).start()

    own_rows = pbuf[me.t]
    moment[...] = column_gram(own_rows, own_rows).reshape(moment.shape)
    me.spread_plane(moment, moment_in, ma_s, ma_r)
    moment_in[me.p] = moment[me.p]

    wacc[...] = jnp.zeros_like(wacc)

    def contribute(t):
        start = pl.multiple_of(t * rows, rows)
        wacc[...] += column_gram(x_ref[pl.ds(start, rows), :], pbuf[t]).reshape(wacc.shape)

    def across(y):
        pass_over(y).wait_recv()
        contribute(me.partner - me.t + me.time_of(y))

    contribute(me.t)
    across(me.y)
    if last:
        def square(k, carry):
            start = pl.multiple_of(k * 64, 64)
            piece = x_ref[pl.ds(start, 64), :].astype(F32)
            piece = jnp.sum((piece * piece).reshape(8, 8, piece.shape[1]), axis=0)
            return carry + piece[:, : carry.shape[1]] + piece[:, carry.shape[1] :]

        square_ref[...] = lax.fori_loop(
            0, x_ref.shape[0] // 64, square, jnp.zeros(square_ref.shape, F32)
        )
    up_low.wait_recv()
    far_low = pbuf.at[t_down, low]
    far_up = me.copy(far_low, far_low, gring_s.at[4], gring_r.at[4], t=t_up)
    far_up.start()
    down_high.wait_recv()
    far_high = pbuf.at[t_up, high]
    far_down = me.copy(far_high, far_high, gring_s.at[5], gring_r.at[5], t=t_down)
    far_down.start()

    me.finish_spread(moment, moment_in, ma_s, ma_r)
    moment_own[...] = total_of(moment_in)
    me.share_times(moment_own, moment_times, mb_s, mb_r)
    moment_times[me.t] = moment_own[...]

    up_high.wait_recv()
    pass_over(down).start()
    down_low.wait_recv()
    pass_over(up).start()
    contribute(t_down)
    contribute(t_up)
    across(down)
    across(up)
    me.finish_times(moment_own, moment_times, mb_s, mb_r)
    moment_all[me.p] = total_of(moment_times)
    me.share_plane(moment_all.at[me.p], moment_all, mc_s, mc_r)
    far_up.wait_recv()
    far_down.wait_recv()
    pass_over(far).start()
    contribute(t_far)
    across(far)

    me.spread_plane(wacc, winc, w_s, w_r)
    winc[me.p] = wacc[me.p]
    if last:
        all_ref[...] = pbuf[...]
    me.finish_plane(gram_all.at[me.p], gram_all, gb_s, gb_r)
    g_ref[...] = gram_all[...].reshape(g_ref.shape)
    me.finish_plane(moment_all.at[me.p], moment_all, mc_s, mc_r)
    m_ref[...] = moment_all[...].reshape(m_ref.shape)
    me.finish_spread(wacc, winc, w_s, w_r)
    w_ref[...] = total_of(winc)

    for sent in (relay_up, relay_down, direct_up, direct_down, joined_up, joined_down):
        sent.wait_send()
    for sent in (up_low, down_high, up_high, down_low, far_up, far_down):
        sent.wait_send()
    for y in range(ring):
        to_pair(y).wait_send()
        pass_over(y).wait_send()


def sweep(data, factors, first, last):
    planes, times = lax.axis_size("series"), lax.axis_size("tm")
    ring = times // 2
    n = factors.shape[1]
    span = data.shape[1]
    rows = data.shape[0] // times
    half = rows // 2
    slab, tall = n // planes, span // planes
    out_shape = [
        jax.ShapeDtypeStruct((tall, n), F32),
        jax.ShapeDtypeStruct((n, n), F32),
        jax.ShapeDtypeStruct((n, n), F32),
    ]
    if last:
        out_shape += [
            jax.ShapeDtypeStruct((times, rows, n), BF16),
            jax.ShapeDtypeStruct((8, n), F32),
        ]
    scratch = []
    if first:
        out_shape += [jax.ShapeDtypeStruct(data.shape, BF16)]
        scratch += [DMA]
    else:
        scratch += [pltpu.VMEM((planes, tall, n), BF16), DMA((planes,)), DMA((planes,))]
    scratch += [pltpu.VMEM((ring, rows, n), BF16)] * 3 + [pltpu.VMEM((ring, rows, n), F32)]
    scratch += [pltpu.VMEM((2, half, n), BF16)] * 4
    scratch += [
        pltpu.VMEM((n, n), F32),
        pltpu.VMEM((times, slab, n), F32),
        pltpu.VMEM((planes, slab, n), F32),
        pltpu.VMEM((planes, slab, n), F32),
        pltpu.VMEM((planes, slab, n), F32),
        pltpu.VMEM((slab, n), F32),
        pltpu.VMEM((times, slab, n), F32),
        pltpu.VMEM((planes, slab, n), F32),
        pltpu.VMEM((times, rows, n), BF16),
        pltpu.VMEM((planes, tall, n), F32),
        pltpu.VMEM((planes, tall, n), F32),
    ]
    scratch += [DMA((ring,)), DMA((ring,)), DMA((6,)), DMA((6,))]
    scratch += [DMA((times,)), DMA((times,)), DMA((planes,)), DMA((planes,))]
    scratch += [DMA((ring,)), DMA((ring,)), DMA((6,)), DMA((6,))]
    scratch += [DMA((planes,)), DMA((planes,)), DMA((times,)), DMA((times,))]
    scratch += [DMA((planes,)), DMA((planes,)), DMA((planes,)), DMA((planes,))]
    return pl.pallas_call(
        functools.partial(sweep_kernel, first, last),
        out_shape=tuple(out_shape),
        in_specs=[pl.BlockSpec(memory_space=pltpu.HBM if first else pltpu.VMEM), *in_vmem(1)],
        out_specs=tuple(in_vmem(len(out_shape))),
        scratch_shapes=scratch,
        compiler_params=pltpu.CompilerParams(
            collective_id=0 if first else 2 if last else 1,
            has_side_effects=True,
            vmem_limit_bytes=(48 if first else 32) * 1024 * 1024,
        ),
        name="sweep_first" if first else "sweep_last" if last else "sweep",
    )(data, factors)


def regularized(gram):
    shape = gram.shape
    diagonal = lax.broadcasted_iota(jnp.int32, shape, 0) == lax.broadcasted_iota(jnp.int32, shape, 1)
    return gram + jnp.where(diagonal, RIDGE, 0.0)


def next_factors(w_ref, inverse, ridged):
    return wide(wide(w_ref[...], inverse), ridged).astype(BF16)


def solve_kernel(w_ref, m_ref, g_ref, f_ref, *state):
    ridged = regularized(g_ref[...])
    (inverse,) = inverses_of([m_ref[...] + RIDGE * wide(ridged, ridged)], *state)
    f_ref[...] = next_factors(w_ref, inverse, ridged)


def solve_last_kernel(w_ref, m_ref, g_ref, f_ref, inverse_ref, *state):
    ridged = regularized(g_ref[...])
    combined = m_ref[...] + RIDGE * wide(ridged, ridged)
    inverse, inverse_ref[...] = inverses_of([combined, ridged], *state)
    f_ref[...] = next_factors(w_ref, inverse, ridged)


def solve(cross, moment, gram, last):
    factors = jax.ShapeDtypeStruct(cross.shape, BF16)
    square = jax.ShapeDtypeStruct(gram.shape, F32)
    return pl.pallas_call(
        solve_last_kernel if last else solve_kernel,
        out_shape=(factors, square) if last else (factors,),
        in_specs=in_vmem(3),
        out_specs=tuple(in_vmem(2 if last else 1)),
        scratch_shapes=squares_of(2 if last else 1, gram.shape[0]),
        compiler_params=pltpu.CompilerParams(vmem_limit_bytes=16 * 1024 * 1024),
        name="solve_last" if last else "solve",
    )(cross, moment, gram)


def folded(rows):
    rows = jnp.sum(rows.reshape(rows.shape[0] // 8, 8, rows.shape[1]), axis=0)
    side = rows.shape[1] // 2
    return rows[:, :side] + rows[:, side:]


def tail_kernel(
    f_ref, w_ref, m_ref, inverse_ref, p_ref, square_ref,
    all_ref, lag_ref, base_ref, earlier_ref, sums_ref, l_ref,
    top, middle, bottom, fbuf, before, lag, base, message, message_in, message_all,
    f_s, f_r, row_s, row_r, ta_s, ta_r, tb_s, tb_r,
):
    me = Place()
    span, n = all_ref.shape
    edge = before.shape[0]
    me.greet(me.time_others() + me.plane_others())
    me.share_plane(f_ref, fbuf, f_s, f_r)
    fbuf[me.p] = f_ref[...]
    slab = n // me.planes

    inverse = inverse_ref[...]
    known = f_ref[...].astype(F32)
    quadratic = wide(wide(inverse, m_ref[...]), inverse)
    side = n // 2
    message[2 * slab :, :side] = folded(wide(known, quadratic) * known) - 2.0 * folded(
        wide(known, inverse) * w_ref[...]
    )
    message[2 * slab :, side:] = folded(square_ref[...])
    top[...] = inverse.astype(BF16)
    rest = inverse - top[...].astype(F32)
    middle[...] = rest.astype(BF16)
    bottom[...] = (rest - middle[...].astype(F32)).astype(BF16)

    def load(k, carry):
        rows = p_ref[k]
        parts = narrow(rows, bottom[...]) + narrow(rows, middle[...]) + narrow(rows, top[...])
        l_ref[k] = parts.astype(BF16)
        return carry

    count = p_ref.shape[0]
    lax.fori_loop(0, count // 4, load, 0)
    me.finish_plane(f_ref, fbuf, f_s, f_r)
    following = lax.rem(me.t + 1, me.times)
    last_rows = fbuf.at[me.planes - 1, pl.ds(fbuf.shape[1] - edge, edge)]
    row = me.copy(last_rows, before, row_s, row_r, t=following)
    row.start()
    factors = fbuf[...].reshape(span, n)
    all_ref[...] = factors
    rolled = pltpu.roll(factors.astype(F32), 1, 0)
    first = lax.broadcasted_iota(jnp.int32, (span, n), 0) == 0
    row.wait()
    head = before[...].astype(F32)[edge - 1 :, :]
    head = head * jnp.where(me.t == 0, 0.0, 1.0)
    earlier = jnp.where(first, head, rolled).astype(BF16)
    earlier_ref[...] = earlier
    lag[...] = column_gram(factors, earlier)
    base[...] = column_gram(earlier, earlier)
    here = pl.ds(pl.multiple_of(me.p * slab, slab), slab)
    message[:slab, :] = lag[here, :]
    message[slab : 2 * slab, :] = base[here, :]
    me.share_times(message, message_in, ta_s, ta_r)
    message_in[me.t] = message[...]
    lax.fori_loop(count // 4, count // 2, load, 0)
    me.finish_times(message, message_in, ta_s, ta_r)
    message_all[me.p] = total_of(message_in)
    me.share_plane(message_all.at[me.p], message_all, tb_s, tb_r)
    lax.fori_loop(count // 2, count, load, 0)
    me.finish_plane(message_all.at[me.p], message_all, tb_s, tb_r)
    lag_ref[...] = message_all[:, :slab, :].reshape(n, n)
    base_ref[...] = message_all[:, slab : 2 * slab, :].reshape(n, n)
    sums_ref[...] = total_of(message_all[:, 2 * slab :, :])


def tail(factors, cross, moment, inverse, projection, squares):
    planes, times = lax.axis_size("series"), lax.axis_size("tm")
    slab, n = factors.shape
    span = slab * planes
    tall = 2 * (n // planes) + squares.shape[0]
    square = jax.ShapeDtypeStruct((n, n), F32)
    block = jax.ShapeDtypeStruct((span, n), BF16)
    sums = jax.ShapeDtypeStruct(squares.shape, F32)
    return pl.pallas_call(
        tail_kernel,
        out_shape=(
            block, square, square, block, sums, jax.ShapeDtypeStruct(projection.shape, BF16)
        ),
        in_specs=in_vmem(6),
        out_specs=tuple(in_vmem(6)),
        scratch_shapes=[
            pltpu.VMEM((n, n), BF16),
            pltpu.VMEM((n, n), BF16),
            pltpu.VMEM((n, n), BF16),
            pltpu.VMEM((planes, slab, n), BF16),
            pltpu.VMEM((16, n), BF16),
            pltpu.VMEM((n, n), F32),
            pltpu.VMEM((n, n), F32),
            pltpu.VMEM((tall, n), F32),
            pltpu.VMEM((times, tall, n), F32),
            pltpu.VMEM((planes, tall, n), F32),
            DMA((planes,)), DMA((planes,)), DMA, DMA,
            DMA((times,)), DMA((times,)), DMA((planes,)), DMA((planes,)),
        ],
        compiler_params=pltpu.CompilerParams(
            collective_id=3, has_side_effects=True, vmem_limit_bytes=32 * 1024 * 1024
        ),
        name="tail",
    )(factors, cross, moment, inverse, projection, squares)


def fit_kernel(
    lag_ref, base_ref, f_ref, earlier_ref, sums_ref, l_ref,
    move_ref, news_ref, factors_ref, share_ref, loadings_ref, a_ref, x_ref, e_ref, sem,
):
    saved = pltpu.make_async_copy(l_ref, loadings_ref, sem)
    saved.start()
    (inverse,) = inverses_of([regularized(base_ref[...])], a_ref, x_ref, e_ref)
    move = wide(lag_ref[...], inverse)
    move_ref[...] = move
    predicted = lax.dot_general(
        earlier_ref[...].astype(F32),
        move,
        (((1,), (1,)), ((), ())),
        precision=lax.Precision.HIGHEST,
        preferred_element_type=F32,
    )
    news_ref[...] = f_ref[...].astype(F32) - predicted
    factors_ref[...] = f_ref[...]
    side = sums_ref.shape[1] // 2
    total = jnp.sum(sums_ref[:, side:])
    share_ref[0, 0] = (total + jnp.sum(sums_ref[:, :side])) / total
    saved.wait()


def fit(lagged, base, factors, earlier, sums, loadings):
    span, n = factors.shape
    return pl.pallas_call(
        fit_kernel,
        out_shape=(
            jax.ShapeDtypeStruct((n, n), F32),
            jax.ShapeDtypeStruct((span, n), F32),
            jax.ShapeDtypeStruct((span, n), BF16),
            jax.ShapeDtypeStruct((1, 1), F32),
            jax.ShapeDtypeStruct(loadings.shape, BF16),
        ),
        in_specs=in_vmem(6),
        out_specs=(
            *in_vmem(3),
            pl.BlockSpec(memory_space=pltpu.SMEM),
            pl.BlockSpec(memory_space=pltpu.HBM),
        ),
        scratch_shapes=squares_of(1, n) + [DMA],
        compiler_params=pltpu.CompilerParams(vmem_limit_bytes=16 * 1024 * 1024),
        name="fit",
    )(lagged, base, factors, earlier, sums, loadings)


def body(data, factors_init):
    factors, held = factors_init, data
    for step in range(ITERS):
        first, last = step == 0, step == ITERS - 1
        cross, moment, gram, *extra = sweep(held, factors, first, last)
        if first:
            (held,) = extra
        factors, *inverse = solve(cross, moment, gram, last)
    projection, squares = extra
    gathered, lagged, base, earlier, sums, loadings = tail(
        factors, cross, moment, *inverse, projection, squares
    )
    transition, innovations, factors, share, loadings = fit(
        lagged, base, gathered, earlier, sums, loadings
    )
    loadings = loadings.reshape(data.shape[0], factors.shape[1])
    return (loadings, factors, innovations, transition, share.reshape(()))


def solution(mesh):
    return jax.shard_map(
        body,
        mesh=mesh,
        in_specs=(P("series", "tm"), P("tm", None)),
        out_specs=(P("series", None), P("tm", None), P("tm", None), P(), P()),
        check_vma=False,
    )
```

```python
import functools
import math

import jax
import jax.numpy as jnp
from jax import lax
from jax.experimental import pallas as pl
from jax.experimental.pallas import tpu as pltpu
from jax.sharding import PartitionSpec as P

ITERS = 3
RIDGE = 0.01
MESH = pl.DeviceIdType.MESH
F32 = jnp.float32
BF16 = jnp.bfloat16
DMA = pltpu.SemaphoreType.DMA


def narrow(left, right):
    return jnp.dot(left.astype(BF16), right.astype(BF16), preferred_element_type=F32)


def wide(left, right):
    return jnp.dot(left, right, precision=lax.Precision.HIGHEST, preferred_element_type=F32)


def column_gram(left, right):
    return lax.dot_general(left, right, (((0,), (0,)), ((), ())), preferred_element_type=F32)


def inverses_of(grams, a_ref, x_ref, e_ref):
    n = grams[0].shape[0]
    each = range(len(grams))
    rows = lax.broadcasted_iota(jnp.int32, (n, n), 0)
    cols = lax.broadcasted_iota(jnp.int32, (n, n), 1)
    diagonal = rows == cols
    down, across, alpha = [], [], []
    for i in each:
        masked = jnp.where(diagonal, grams[i], 0.0)
        down.append(lax.rsqrt(jnp.sum(masked, axis=1, keepdims=True)))
        across.append(lax.rsqrt(jnp.sum(masked, axis=0, keepdims=True)))
        scaled = grams[i] * down[i] * across[i]
        a_ref[i] = scaled
        alpha.append(1.9 / jnp.max(jnp.sum(jnp.abs(scaled), axis=0, keepdims=True)))
        x_ref[i] = jnp.where(diagonal, alpha[i], 0.0)
        e_ref[i] = jnp.where(diagonal, 1.0, 0.0) - alpha[i] * scaled

    def worst_of(values):
        return functools.reduce(jnp.maximum, values)

    def squaring(carry):
        step, _ = carry
        for _ in range(2):
            for i in each:
                error = e_ref[i]
                guess = x_ref[i]
                e_ref[i] = narrow(error, error)
                x_ref[i] = guess + narrow(guess, error)
        return step + 1, worst_of([jnp.sum(e_ref[i] * e_ref[i]) for i in each])

    lax.while_loop(
        lambda c: jnp.logical_and(c[0] < 10, jnp.logical_and(c[1] > 1e-2, c[1] < 1e3)),
        squaring,
        (0, jnp.float32(1.0)),
    )

    def residual():
        for i in each:
            e_ref[i] = jnp.where(diagonal, 1.0, 0.0) - wide(a_ref[i], x_ref[i])
        return worst_of([jnp.max(jnp.abs(e_ref[i])) for i in each])

    def refine(carry):
        step, _ = carry
        worst = residual()
        for i in each:
            guess = x_ref[i]
            x_ref[i] = guess + narrow(guess, e_ref[i])
        return step + 1, worst

    _, worst = lax.while_loop(
        lambda c: jnp.logical_and(c[0] < 8, jnp.logical_and(c[1] >= 5e-4, c[1] < 2.0)),
        refine,
        (0, jnp.float32(1.0)),
    )

    @pl.when(worst >= 5e-4)
    def _():
        for i in each:
            x_ref[i] = jnp.where(diagonal, alpha[i], 0.0)

        def newton(carry):
            step, _ = carry
            error = residual()
            for i in each:
                guess = x_ref[i]
                x_ref[i] = guess + wide(guess, e_ref[i])
            return step + 1, error

        lax.while_loop(
            lambda c: jnp.logical_and(c[0] < 48, c[1] >= 5e-4),
            newton,
            (0, jnp.float32(1.0)),
        )

    return [x_ref[i] * down[i] * across[i] for i in each]


def squares_of(count, n):
    return [pltpu.VMEM((count, n, n), F32)] * 3


class Place:
    def __init__(self):
        self.p = lax.axis_index("series")
        self.t = lax.axis_index("tm")
        self.planes = lax.axis_size("series")
        self.times = lax.axis_size("tm")
        self.ring = self.times // 2
        self.side = math.isqrt(self.planes)
        self.y = lax.div(self.t, 2)
        self.c = lax.rem(self.t, 2)
        self.partner = self.t + 1 - 2 * self.c

    def ring_at(self, distance):
        return lax.rem(self.y + distance, self.ring)

    def time_of(self, y):
        return 2 * y + self.c

    def copy(self, src, dst, send, recv, p=None, t=None):
        return pltpu.make_async_remote_copy(
            src_ref=src,
            dst_ref=dst,
            send_sem=send,
            recv_sem=recv,
            device_id=(self.p if p is None else p, self.t if t is None else t),
            device_id_type=MESH,
        )

    def greet(self, others, meanwhile=None):
        barrier = pltpu.get_barrier_semaphore()
        for p, t in others:
            pl.semaphore_signal(barrier, inc=1, device_id=(p, t), device_id_type=MESH)
        if meanwhile is not None:
            meanwhile()
        pl.semaphore_wait(barrier, len(others))

    def plane_at(self, k):
        side = self.side
        row = lax.rem(lax.div(self.p, side) + k // side, side)
        return row * side + lax.rem(lax.rem(self.p, side) + k % side, side)

    def plane_order(self):
        def hops(k):
            return sum(min(d, self.side - d) for d in divmod(k, self.side))

        return sorted(range(1, self.planes), key=lambda k: -hops(k))

    def plane_others(self):
        return [(self.plane_at(k), self.t) for k in self.plane_order()]

    def time_others(self):
        return [(self.p, lax.rem(self.t + k, self.times)) for k in range(1, self.times)]

    def share_plane(self, message, blocks, send, recv):
        for k in self.plane_order():
            to = self.plane_at(k)
            self.copy(message, blocks.at[self.p], send.at[k], recv.at[self.p], p=to).start()

    def finish_plane(self, message, blocks, send, recv):
        def wait(k, carry):
            other = self.plane_at(k)
            self.copy(message, blocks.at[other], send.at[k], recv.at[other], p=other).wait()
            return carry

        lax.fori_loop(1, self.planes, wait, 0)

    def spread_plane(self, pieces, blocks, send, recv):
        for k in self.plane_order():
            to = self.plane_at(k)
            self.copy(pieces.at[to], blocks.at[self.p], send.at[k], recv.at[self.p], p=to).start()

    def finish_spread(self, pieces, blocks, send, recv):
        def wait(k, carry):
            other = self.plane_at(k)
            self.copy(pieces.at[other], blocks.at[other], send.at[k], recv.at[other], p=other).wait()
            return carry

        lax.fori_loop(1, self.planes, wait, 0)

    def split_times(self, pieces, blocks, send, recv):
        def start(k, carry):
            to = lax.rem(self.t + k, self.times)
            piece = pieces.at[lax.rem(to, 2)]
            self.copy(piece, blocks.at[self.t], send.at[k], recv.at[self.t], t=to).start()
            return carry

        lax.fori_loop(1, self.times, start, 0)

    def swap(self, halves, send, recv):
        mine = halves.at[self.c]
        return self.copy(mine, mine, send, recv, t=self.partner)

    def share_times(self, message, blocks, send, recv):
        def start(k, carry):
            to = lax.rem(self.t + k, self.times)
            self.copy(message, blocks.at[self.t], send.at[k], recv.at[self.t], t=to).start()
            return carry

        lax.fori_loop(1, self.times, start, 0)

    def finish_times(self, message, blocks, send, recv):
        def wait(k, carry):
            other = lax.rem(self.t + k, self.times)
            self.copy(message, blocks.at[other], send.at[k], recv.at[other], t=other).wait()
            return carry

        lax.fori_loop(1, self.times, wait, 0)


def total_of(blocks):
    total = blocks[0]
    for k in range(1, blocks.shape[0]):
        total = total + blocks[k]
    return total


def in_vmem(count):
    return [pl.BlockSpec(memory_space=pltpu.VMEM)] * count


def sweep_kernel(first, last, *refs):
    refs = list(refs)

    def take(count):
        taken, refs[:] = refs[:count], refs[count:]
        return taken

    if first:
        x_ref, f_ref = take(2)
    else:
        x_ref, before_ref, inverse_ref, ridged_ref = take(4)
    w_ref, n_ref, g_ref = take(3)
    if last:
        m_ref, all_ref, square_ref = take(3)
    if first:
        x_from = x_ref
        x_ref, x_sem = take(2)
    else:
        f_ref, fbuf, f_s, f_r = take(4)
    part, other, chip, acc, relay_in, direct_in, relay_out, joined_in = take(8)
    gram, gram_in, gram_all, moment, moment_in, moment_own, moment_times, moment_all = take(8)
    pbuf, wacc, winc = take(3)
    pair_s, pair_r, ring_s, ring_r, ga_s, ga_r, gb_s, gb_r = take(8)
    moment_full, swap_s, swap_r = take(3)
    gpair_s, gpair_r, gring_s, gring_r, ma_s, ma_r, mb_s, mb_r, mc_s, mc_r, w_s, w_r = take(12)
    me = Place()
    rows = acc.shape[1]
    half = rows // 2
    low, high = pl.ds(0, half), pl.ds(half, half)
    ring = me.ring
    up, down, far = me.ring_at(1), me.ring_at(ring - 1), me.ring_at(2)
    t_up, t_down, t_far = me.time_of(up), me.time_of(down), me.time_of(far)
    slab = gram_in.shape[1]

    def bring():
        x_copy = pltpu.make_async_copy(x_from, x_ref, x_sem)
        x_copy.start()
        gram[...] = column_gram(f_ref[...], f_ref[...])
        x_copy.wait()

    def solved():
        f_ref[...] = next_factors(before_ref, inverse_ref[...], ridged_ref[...])

    me.greet(me.time_others() + me.plane_others(), bring if first else solved)

    if first:
        def factors():
            return f_ref[...]
    else:
        me.share_plane(f_ref, fbuf, f_s, f_r)
        fbuf[me.p] = f_ref[...]
        me.finish_plane(f_ref, fbuf, f_s, f_r)

        def factors():
            return fbuf[...].reshape(x_ref.shape[1], f_ref.shape[1])

    if not first:
        gram[...] = column_gram(factors(), factors())
    mine = gram.at[pl.ds(pl.multiple_of(me.p * slab, slab), slab)]
    me.share_times(mine, gram_in, ga_s, ga_r)
    gram_in[me.t] = mine[...]

    def block(owner):
        start = pl.multiple_of(owner * rows, rows)
        return jnp.dot(x_ref[pl.ds(start, rows), :], factors(), preferred_element_type=F32)

    def to_pair(y):
        return me.copy(part.at[y], other.at[y], pair_s.at[y], pair_r.at[y], t=me.partner)

    def give(k, carry):
        y = me.ring_at(2 + 3 * k)
        part[y] = block(me.partner - me.t + me.time_of(y)).astype(BF16)
        to_pair(y).start()
        return carry

    lax.fori_loop(0, ring, give, 0)

    def chip_sum(y):
        own = block(me.time_of(y))
        to_pair(y).wait_recv()
        acc[y] = own + other[y].astype(F32)

    chip_sum(far)
    chip[far] = acc[far].astype(BF16)
    relay_up = me.copy(chip.at[far, low], relay_in.at[0], ring_s.at[0], ring_r.at[0], t=t_up)
    relay_down = me.copy(chip.at[far, high], relay_in.at[1], ring_s.at[1], ring_r.at[1], t=t_down)
    relay_up.start()
    relay_down.start()
    chip_sum(up)
    chip[up, high] = acc[up, high].astype(BF16)
    direct_up = me.copy(chip.at[up, high], direct_in.at[0], ring_s.at[2], ring_r.at[2], t=t_up)
    direct_up.start()
    chip_sum(down)
    chip[down, low] = acc[down, low].astype(BF16)
    direct_down = me.copy(chip.at[down, low], direct_in.at[1], ring_s.at[3], ring_r.at[3], t=t_down)
    direct_down.start()
    chip_sum(me.y)

    relay_up.wait_recv()
    relay_out[0] = (acc[up, low] + relay_in[0].astype(F32)).astype(BF16)
    joined_up = me.copy(relay_out.at[0], joined_in.at[0], ring_s.at[4], ring_r.at[4], t=t_up)
    joined_up.start()
    relay_down.wait_recv()
    relay_out[1] = (acc[down, high] + relay_in[1].astype(F32)).astype(BF16)
    joined_down = me.copy(relay_out.at[1], joined_in.at[1], ring_s.at[5], ring_r.at[5], t=t_down)
    joined_down.start()

    me.finish_times(mine, gram_in, ga_s, ga_r)
    gram_all[me.p] = total_of(gram_in)
    me.share_plane(gram_all.at[me.p], gram_all, gb_s, gb_r)

    direct_up.wait_recv()
    direct_down.wait_recv()
    joined_up.wait_recv()
    pbuf[me.t, low] = (
        acc[me.y, low] + direct_in[1].astype(F32) + joined_in[0].astype(F32)
    ).astype(BF16)
    mine_low, mine_high = pbuf.at[me.t, low], pbuf.at[me.t, high]
    up_low = me.copy(mine_low, mine_low, gring_s.at[0], gring_r.at[0], t=t_up)
    up_low.start()
    joined_down.wait_recv()
    pbuf[me.t, high] = (
        acc[me.y, high] + direct_in[0].astype(F32) + joined_in[1].astype(F32)
    ).astype(BF16)
    down_high = me.copy(mine_high, mine_high, gring_s.at[1], gring_r.at[1], t=t_down)
    down_high.start()
    up_high = me.copy(mine_high, mine_high, gring_s.at[2], gring_r.at[2], t=t_up)
    up_high.start()
    down_low = me.copy(mine_low, mine_low, gring_s.at[3], gring_r.at[3], t=t_down)
    down_low.start()

    def pass_over(y):
        piece = pbuf.at[me.time_of(y)]
        return me.copy(piece, piece, gpair_s.at[y], gpair_r.at[y], t=me.partner)

    pass_over(me.y).start()

    own_rows = pbuf[me.t]
    moment[...] = column_gram(own_rows, own_rows).reshape(moment.shape)
    me.spread_plane(moment, moment_in, ma_s, ma_r)
    moment_in[me.p] = moment[me.p]

    wacc[...] = jnp.zeros_like(wacc)

    def contribute(t):
        start = pl.multiple_of(t * rows, rows)
        wacc[...] += column_gram(x_ref[pl.ds(start, rows), :], pbuf[t]).reshape(wacc.shape)

    def across(y):
        pass_over(y).wait_recv()
        contribute(me.partner - me.t + me.time_of(y))

    contribute(me.t)
    across(me.y)
    if last:
        def square(k, carry):
            start = pl.multiple_of(k * 64, 64)
            piece = x_ref[pl.ds(start, 64), :].astype(F32)
            piece = jnp.sum((piece * piece).reshape(8, 8, piece.shape[1]), axis=0)
            return carry + piece[:, : carry.shape[1]] + piece[:, carry.shape[1] :]

        square_ref[...] = lax.fori_loop(
            0, x_ref.shape[0] // 64, square, jnp.zeros(square_ref.shape, F32)
        )
    up_low.wait_recv()
    far_low = pbuf.at[t_down, low]
    far_up = me.copy(far_low, far_low, gring_s.at[4], gring_r.at[4], t=t_up)
    far_up.start()
    down_high.wait_recv()
    far_high = pbuf.at[t_up, high]
    far_down = me.copy(far_high, far_high, gring_s.at[5], gring_r.at[5], t=t_down)
    far_down.start()

    me.finish_spread(moment, moment_in, ma_s, ma_r)
    moment_own[...] = total_of(moment_in).reshape(moment_own.shape)
    me.split_times(moment_own, moment_times, mb_s, mb_r)
    moment_times[me.t] = moment_own[me.c]

    up_high.wait_recv()
    pass_over(down).start()
    down_low.wait_recv()
    pass_over(up).start()
    contribute(t_down)
    contribute(t_up)
    across(down)
    across(up)
    me.finish_times(moment_own.at[0], moment_times, mb_s, mb_r)
    moment_all[me.c, me.p] = total_of(moment_times)
    moment_mine = moment_all.at[me.c]
    me.share_plane(moment_mine.at[me.p], moment_mine, mc_s, mc_r)
    far_up.wait_recv()
    far_down.wait_recv()
    pass_over(far).start()
    contribute(t_far)
    across(far)

    me.spread_plane(wacc, winc, w_s, w_r)
    winc[me.p] = wacc[me.p]
    if last:
        all_ref[...] = pbuf[...]
    me.finish_plane(gram_all.at[me.p], gram_all, gb_s, gb_r)
    g_ref[...] = regularized(gram_all[...].reshape(g_ref.shape))
    n_ref[...] = RIDGE * wide(g_ref[...], g_ref[...])
    me.finish_plane(moment_mine.at[me.p], moment_mine, mc_s, mc_r)
    swap = me.swap(moment_all, swap_s, swap_r)
    swap.start()
    me.finish_spread(wacc, winc, w_s, w_r)
    w_ref[...] = total_of(winc)
    swap.wait()
    for core in range(2):
        moment_full[:, core] = moment_all[core]
    total = moment_full[...].reshape(n_ref.shape)
    n_ref[...] += total
    if last:
        m_ref[...] = total

    for sent in (relay_up, relay_down, direct_up, direct_down, joined_up, joined_down):
        sent.wait_send()
    for sent in (up_low, down_high, up_high, down_low, far_up, far_down):
        sent.wait_send()
    for y in range(ring):
        to_pair(y).wait_send()
        pass_over(y).wait_send()


def sweep(data, held, first, last):
    planes, times = lax.axis_size("series"), lax.axis_size("tm")
    ring = times // 2
    n = held[0].shape[1]
    span = data.shape[1]
    rows = data.shape[0] // times
    half = rows // 2
    slab, tall = n // planes, span // planes
    out_shape = [
        jax.ShapeDtypeStruct((tall, n), F32),
        jax.ShapeDtypeStruct((n, n), F32),
        jax.ShapeDtypeStruct((n, n), F32),
    ]
    if last:
        out_shape += [
            jax.ShapeDtypeStruct((n, n), F32),
            jax.ShapeDtypeStruct((times, rows, n), BF16),
            jax.ShapeDtypeStruct((8, n), F32),
        ]
    scratch = []
    if first:
        out_shape += [jax.ShapeDtypeStruct(data.shape, BF16)]
        scratch += [DMA]
    else:
        scratch += [pltpu.VMEM((tall, n), BF16), pltpu.VMEM((planes, tall, n), BF16)]
        scratch += [DMA((planes,)), DMA((planes,))]
    scratch += [pltpu.VMEM((ring, rows, n), BF16)] * 3 + [pltpu.VMEM((ring, rows, n), F32)]
    scratch += [pltpu.VMEM((2, half, n), BF16)] * 4
    scratch += [
        pltpu.VMEM((n, n), F32),
        pltpu.VMEM((times, slab, n), F32),
        pltpu.VMEM((planes, slab, n), F32),
        pltpu.VMEM((planes, slab, n), F32),
        pltpu.VMEM((planes, slab, n), F32),
        pltpu.VMEM((2, slab // 2, n), F32),
        pltpu.VMEM((times, slab // 2, n), F32),
        pltpu.VMEM((2, planes, slab // 2, n), F32),
        pltpu.VMEM((times, rows, n), BF16),
        pltpu.VMEM((planes, tall, n), F32),
        pltpu.VMEM((planes, tall, n), F32),
    ]
    scratch += [DMA((ring,)), DMA((ring,)), DMA((6,)), DMA((6,))]
    scratch += [DMA((times,)), DMA((times,)), DMA((planes,)), DMA((planes,))]
    scratch += [pltpu.VMEM((planes, 2, slab // 2, n), F32), DMA, DMA]
    scratch += [DMA((ring,)), DMA((ring,)), DMA((6,)), DMA((6,))]
    scratch += [DMA((planes,)), DMA((planes,)), DMA((times,)), DMA((times,))]
    scratch += [DMA((planes,)), DMA((planes,)), DMA((planes,)), DMA((planes,))]
    return pl.pallas_call(
        functools.partial(sweep_kernel, first, last),
        out_shape=tuple(out_shape),
        in_specs=[
            pl.BlockSpec(memory_space=pltpu.HBM if first else pltpu.VMEM), *in_vmem(len(held))
        ],
        out_specs=tuple(in_vmem(len(out_shape))),
        scratch_shapes=scratch,
        compiler_params=pltpu.CompilerParams(
            collective_id=0 if first else 2 if last else 1,
            has_side_effects=True,
            vmem_limit_bytes=(48 if first else 32) * 1024 * 1024,
        ),
        name="sweep_first" if first else "sweep_last" if last else "sweep",
    )(data, *held)


def regularized(gram):
    shape = gram.shape
    diagonal = lax.broadcasted_iota(jnp.int32, shape, 0) == lax.broadcasted_iota(jnp.int32, shape, 1)
    return gram + jnp.where(diagonal, RIDGE, 0.0)


def next_factors(w_ref, inverse, ridged):
    return wide(wide(w_ref[...], inverse), ridged).astype(BF16)


def solve_kernel(count, *refs):
    grams, inverses, state = refs[:count], refs[count : 2 * count], refs[2 * count :]
    for ref, inverse in zip(inverses, inverses_of([g[...] for g in grams], *state)):
        ref[...] = inverse


def solve(*grams):
    count = len(grams)
    square = jax.ShapeDtypeStruct(grams[0].shape, F32)
    return pl.pallas_call(
        functools.partial(solve_kernel, count),
        out_shape=(square,) * count,
        in_specs=in_vmem(count),
        out_specs=tuple(in_vmem(count)),
        scratch_shapes=squares_of(count, square.shape[0]),
        compiler_params=pltpu.CompilerParams(vmem_limit_bytes=16 * 1024 * 1024),
        name="solve" if count == 1 else "solve_both",
    )(*grams)


def folded(rows):
    rows = jnp.sum(rows.reshape(rows.shape[0] // 8, 8, rows.shape[1]), axis=0)
    side = rows.shape[1] // 2
    return rows[:, :side] + rows[:, side:]


def tail_kernel(
    w_ref, combined_ref, ridged_ref, m_ref, inverse_ref, p_ref, square_ref,
    all_ref, lag_ref, base_ref, earlier_ref, sums_ref, l_ref,
    f_ref, top, middle, bottom, fbuf, before, lag, base, message, message_in, message_all, whole,
    f_s, f_r, row_s, row_r, ta_s, ta_r, tb_s, tb_r, swap_s, swap_r,
):
    me = Place()
    span, n = all_ref.shape
    edge = before.shape[0]

    def solved():
        f_ref[...] = next_factors(w_ref, combined_ref[...], ridged_ref[...])

    me.greet(me.time_others() + me.plane_others(), solved)
    me.share_plane(f_ref, fbuf, f_s, f_r)
    fbuf[me.p] = f_ref[...]
    slab = n // me.planes
    part = slab // 2

    inverse = inverse_ref[...]
    known = f_ref[...].astype(F32)
    quadratic = wide(wide(inverse, m_ref[...]), inverse)
    side = n // 2
    terms = folded(wide(known, quadratic) * known) - 2.0 * folded(
        wide(known, inverse) * w_ref[...]
    )
    squared = folded(square_ref[...])
    for core in range(2):
        message[core, slab:, :side] = terms
        message[core, slab:, side:] = squared
    top[...] = inverse.astype(BF16)
    rest = inverse - top[...].astype(F32)
    middle[...] = rest.astype(BF16)
    bottom[...] = (rest - middle[...].astype(F32)).astype(BF16)

    def load(k, carry):
        rows = p_ref[k]
        parts = narrow(rows, bottom[...]) + narrow(rows, middle[...]) + narrow(rows, top[...])
        l_ref[k] = parts.astype(BF16)
        return carry

    count = p_ref.shape[0]
    lax.fori_loop(0, count // 4, load, 0)
    me.finish_plane(f_ref, fbuf, f_s, f_r)
    following = lax.rem(me.t + 1, me.times)
    last_rows = fbuf.at[me.planes - 1, pl.ds(fbuf.shape[1] - edge, edge)]
    row = me.copy(last_rows, before, row_s, row_r, t=following)
    row.start()
    factors = fbuf[...].reshape(span, n)
    all_ref[...] = factors
    rolled = pltpu.roll(factors.astype(F32), 1, 0)
    first = lax.broadcasted_iota(jnp.int32, (span, n), 0) == 0
    row.wait()
    head = before[...].astype(F32)[edge - 1 :, :]
    head = head * jnp.where(me.t == 0, 0.0, 1.0)
    earlier = jnp.where(first, head, rolled).astype(BF16)
    earlier_ref[...] = earlier
    lag[...] = column_gram(factors, earlier)
    base[...] = column_gram(earlier, earlier)
    for core in range(2):
        here = pl.ds(pl.multiple_of(me.p * slab + core * part, part), part)
        message[core, :part, :] = lag[here, :]
        message[core, part:slab, :] = base[here, :]
    me.split_times(message, message_in, ta_s, ta_r)
    message_in[me.t] = message[me.c]
    lax.fori_loop(count // 4, count // 2, load, 0)
    me.finish_times(message.at[0], message_in, ta_s, ta_r)
    message_all[me.c, me.p] = total_of(message_in)
    message_mine = message_all.at[me.c]
    me.share_plane(message_mine.at[me.p], message_mine, tb_s, tb_r)
    lax.fori_loop(count // 2, count, load, 0)
    me.finish_plane(message_mine.at[me.p], message_mine, tb_s, tb_r)
    swap = me.swap(message_all, swap_s, swap_r)
    swap.start()
    swap.wait()
    for core in range(2):
        whole[0, :, core] = message_all[core, :, :part, :]
        whole[1, :, core] = message_all[core, :, part:slab, :]
    lag_ref[...] = whole[0].reshape(n, n)
    base_ref[...] = whole[1].reshape(n, n)
    sums_ref[...] = total_of(message_all[0, :, slab:, :])


def tail(cross, combined, ridged, moment, inverse, projection, squares):
    planes, times = lax.axis_size("series"), lax.axis_size("tm")
    slab, n = cross.shape
    span = slab * planes
    tall = n // planes + squares.shape[0]
    square = jax.ShapeDtypeStruct((n, n), F32)
    block = jax.ShapeDtypeStruct((span, n), BF16)
    sums = jax.ShapeDtypeStruct(squares.shape, F32)
    return pl.pallas_call(
        tail_kernel,
        out_shape=(
            block, square, square, block, sums, jax.ShapeDtypeStruct(projection.shape, BF16)
        ),
        in_specs=in_vmem(7),
        out_specs=tuple(in_vmem(6)),
        scratch_shapes=[
            pltpu.VMEM((slab, n), BF16),
            pltpu.VMEM((n, n), BF16),
            pltpu.VMEM((n, n), BF16),
            pltpu.VMEM((n, n), BF16),
            pltpu.VMEM((planes, slab, n), BF16),
            pltpu.VMEM((16, n), BF16),
            pltpu.VMEM((n, n), F32),
            pltpu.VMEM((n, n), F32),
            pltpu.VMEM((2, tall, n), F32),
            pltpu.VMEM((times, tall, n), F32),
            pltpu.VMEM((2, planes, tall, n), F32),
            pltpu.VMEM((2, planes, 2, n // planes // 2, n), F32),
            DMA((planes,)), DMA((planes,)), DMA, DMA,
            DMA((times,)), DMA((times,)), DMA((planes,)), DMA((planes,)), DMA, DMA,
        ],
        compiler_params=pltpu.CompilerParams(
            collective_id=3, has_side_effects=True, vmem_limit_bytes=32 * 1024 * 1024
        ),
        name="tail",
    )(cross, combined, ridged, moment, inverse, projection, squares)


def fit_kernel(
    lag_ref, base_ref, f_ref, earlier_ref, sums_ref, l_ref,
    move_ref, news_ref, factors_ref, share_ref, loadings_ref, a_ref, x_ref, e_ref, sem,
):
    saved = pltpu.make_async_copy(l_ref, loadings_ref, sem)
    saved.start()
    (inverse,) = inverses_of([regularized(base_ref[...])], a_ref, x_ref, e_ref)
    move = wide(lag_ref[...], inverse)
    move_ref[...] = move
    predicted = lax.dot_general(
        earlier_ref[...].astype(F32),
        move,
        (((1,), (1,)), ((), ())),
        precision=lax.Precision.HIGHEST,
        preferred_element_type=F32,
    )
    news_ref[...] = f_ref[...].astype(F32) - predicted
    factors_ref[...] = f_ref[...]
    side = sums_ref.shape[1] // 2
    total = jnp.sum(sums_ref[:, side:])
    share_ref[0, 0] = (total + jnp.sum(sums_ref[:, :side])) / total
    saved.wait()


def fit(lagged, base, factors, earlier, sums, loadings):
    span, n = factors.shape
    return pl.pallas_call(
        fit_kernel,
        out_shape=(
            jax.ShapeDtypeStruct((n, n), F32),
            jax.ShapeDtypeStruct((span, n), F32),
            jax.ShapeDtypeStruct((span, n), BF16),
            jax.ShapeDtypeStruct((1, 1), F32),
            jax.ShapeDtypeStruct(loadings.shape, BF16),
        ),
        in_specs=in_vmem(6),
        out_specs=(
            *in_vmem(3),
            pl.BlockSpec(memory_space=pltpu.SMEM),
            pl.BlockSpec(memory_space=pltpu.HBM),
        ),
        scratch_shapes=squares_of(1, n) + [DMA],
        compiler_params=pltpu.CompilerParams(vmem_limit_bytes=16 * 1024 * 1024),
        name="fit",
    )(lagged, base, factors, earlier, sums, loadings)


def body(data, factors_init):
    held, here = (factors_init,), data
    for step in range(ITERS):
        first, last = step == 0, step == ITERS - 1
        cross, combined, ridged, *extra = sweep(here, held, first, last)
        if first:
            (here,) = extra
        if not last:
            held = (cross, *solve(combined), ridged)
    moment, projection, squares = extra
    combined, inverse = solve(combined, ridged)
    gathered, lagged, base, earlier, sums, loadings = tail(
        cross, combined, ridged, moment, inverse, projection, squares
    )
    transition, innovations, factors, share, loadings = fit(
        lagged, base, gathered, earlier, sums, loadings
    )
    loadings = loadings.reshape(data.shape[0], factors.shape[1])
    return (loadings, factors, innovations, transition, share.reshape(()))


def solution(mesh):
    return jax.shard_map(
        body,
        mesh=mesh,
        in_specs=(P("series", "tm"), P("tm", None)),
        out_specs=(P("series", None), P("tm", None), P("tm", None), P(), P()),
        check_vma=False,
    )
```
